256 devices in a mesh: ctx: 32 (over z, y), tp: 8 (over x, core).
Axes of the slice: x: 4, y: 4, z: 8, core: 2. Of those that a mesh axis runs over, the one named last changes fastest.
Arguments:
- queries: bfloat16 [8192, 64, 128], P('ctx', 'tp'), may hold values from -48 to 48
- keys: bfloat16 [8192, 8, 128], P('ctx', 'tp'), may hold values from -3 to 3
- values: bfloat16 [8192, 8, 128], P('ctx', 'tp'), may hold values from -6 to 6
- segment_ids: int32 [8192], P('ctx'), may hold values from 0 to 7, never falling along the last dimension, each value on 1 to 5120 neighbouring positions
Outputs:
- attended: bfloat16 [8192, 8192], P(('ctx', 'tp'))
The draws below stay inside these ranges and needn't reach their ends.
Inputs may be any that keep to these rules, and one draw needn't show every extreme that they name: `segment_ids`: ids never fall along the tokens; each document holds 1 to 5120 tokens, and one holds exactly 5120.
All inputs are finite; a program needn't handle non-finite values.
Results may differ from the reference program's by a relative error of at most 0.003.
Values may be sent and summed in bfloat16 or wider, within the bound.
A program may use at most 64 MiB of HBM per device.

```python
import math
import jax
import jax.numpy as jnp
import numpy as np
from jax import lax

QUERY_HEADS = 64
KEY_VALUE_HEADS = 8
HEAD_SIZE = 128
DOCS = 8
PACK_TOKENS = 8192
MOST = 5120


def paired_draw(key):
    base = jax.random.fold_in(key, 4242)
    key_random_keys, key_query = jax.random.split(base, 2)
    keys = jnp.clip(jax.random.normal(key_random_keys, (PACK_TOKENS, KEY_VALUE_HEADS, HEAD_SIZE), jnp.float32), -3.0, 3.0)
    queries = jnp.clip(2.5 * jax.random.normal(key_query, (PACK_TOKENS, QUERY_HEADS, HEAD_SIZE), jnp.float32), -12.0, 12.0)
    return (queries.astype(jnp.bfloat16), keys.astype(jnp.bfloat16))


def draw_queries(key, part):
    return paired_draw(key)[0]


def draw_keys(key, part):
    return paired_draw(key)[1]


def shard_levels(own_key, extent, cuts, least, high):
    loudness, own = 1.0, jax.random.fold_in(own_key, 6)
    for position, shards_of in cuts:
        heights = jnp.exp(jax.random.uniform(jax.random.fold_in(own, position), (shards_of,), jnp.float32, least / len(cuts), high / len(cuts)))
        loudness = loudness * jnp.repeat(heights, extent[position] // shards_of).reshape([-1 if axis == position else 1 for axis in range(len(extent))])
    return loudness


def length_profile(count, total, most, lean):
    weights = [(1 << 20) // math.isqrt(standing ** lean) + 1 for standing in range(2, count + 1)]
    spare, given = total - most - (count - 1), [1] * (count - 1)
    while spare > 0:
        free = [i for i in range(count - 1) if given[i] < most]
        mass, remaining = sum([weights[i] for i in free]), spare
        for i in free:
            addition = min(most - given[i], max(1, remaining * weights[i] // mass), spare)
            given[i] = given[i] + addition
            spare = spare - addition
    return np.array([most] + given)


def uneven(rng, amount, total, limit, skew):
    if amount == 2:
        one = jax.random.randint(rng, (), max(1, total - limit), min(limit, total - 1) + 1)
        return jnp.stack([one, total - one])
    lengths = jnp.asarray(length_profile(amount, total, limit, skew), jnp.int32)
    couples = (amount - 1) // 2
    donor, taker = lengths[1:1 + 2 * couples:2], lengths[2:2 + 2 * couples:2]
    room = jnp.minimum(donor - 1, limit - taker)
    moved = jax.random.randint(jax.random.fold_in(rng, 1), (couples,), 0, 1 << 20) % (room + 1)
    lengths = lengths.at[1:1 + 2 * couples:2].set(donor - moved).at[2:2 + 2 * couples:2].set(taker + moved)
    return lengths[jax.random.permutation(jax.random.fold_in(rng, 2), amount)]


def scatter_about(key, extent, deviation, limit, shards=(), kind=jnp.bfloat16):
    gain = shard_levels(key, extent, shards, -0.22, 0.18) if shards else 1.0
    values = jax.random.normal(key, extent, jnp.float32) * deviation * gain
    return jnp.minimum(jnp.maximum(values, -limit), limit).astype(kind)


def setup_inputs(seed: int = 0) -> dict:
    arg_keys = jax.random.split(jax.random.key(seed), 5)
    return {
        "queries": draw_queries(jax.random.fold_in(arg_keys[4], 71), 0),
        "keys": draw_keys(jax.random.fold_in(arg_keys[4], 71), 0),
        "values": scatter_about(arg_keys[2], (PACK_TOKENS, KEY_VALUE_HEADS, HEAD_SIZE), 1.0, 6.0, ((0, 32), (1, 8))),
        "segment_ids": jnp.searchsorted(jnp.cumsum(uneven(arg_keys[3], DOCS, PACK_TOKENS, MOST, 2)), jnp.arange(PACK_TOKENS), side="right").astype(jnp.int32),
    }


def reference(queries, keys, values, segment_ids):
    tokens, heads, head = queries.shape
    groups = keys.shape[1]
    per_group = heads // groups
    block = math.gcd(tokens, 512)
    positions = jnp.arange(tokens, dtype=jnp.int32)
    scale = 1.0 / math.sqrt(head)

    def one_block(index):
        first = (index * block).astype(jnp.int32)
        query_rows = lax.dynamic_slice_in_dim(queries, first, block, 0).reshape(block, groups, per_group, head)
        seg_rows = lax.dynamic_slice_in_dim(segment_ids, first, block, 0)
        pos_rows = first + jnp.arange(block, dtype=jnp.int32)
        allowed = (seg_rows[:, None] == segment_ids[None, :]) & (positions[None, :] <= pos_rows[:, None])

        def one_group(group):
            query_group = lax.dynamic_index_in_dim(query_rows, group, 1, keepdims=False).astype(jnp.float32)
            key_group = lax.dynamic_index_in_dim(keys, group, 1, keepdims=False).astype(jnp.float32)
            value_group = lax.dynamic_index_in_dim(values, group, 1, keepdims=False).astype(jnp.float32)
            scores = jnp.einsum('tgd,pd->gtp', query_group, key_group) * scale
            scores = jnp.where(allowed[None], scores, -1e+30)
            top = lax.optimization_barrier(jnp.max(scores, axis=-1))
            weights = jnp.where(allowed[None], jnp.exp(scores - top[..., None]), 0.0)
            total = lax.optimization_barrier(jnp.sum(weights, axis=-1))
            rounded = lax.optimization_barrier(weights.astype(jnp.bfloat16)).astype(jnp.float32)
            mixed = jnp.einsum('gtp,pd->gtd', rounded, value_group)
            return mixed / total[..., None]
        result = lax.map(one_group, jnp.arange(groups, dtype=jnp.int32))
        return jnp.transpose(result, (2, 0, 1, 3)).reshape(block, heads * head).astype(jnp.bfloat16)
    output = lax.map(one_block, jnp.arange(tokens // block, dtype=jnp.int32))
    return output.reshape(tokens, heads * head)
```

```python
import functools
import math

import jax
import jax.numpy as jnp
from jax import lax
from jax.experimental import pallas as pl
from jax.experimental.pallas import tpu as pltpu
from jax.sharding import PartitionSpec as P

MESH = pl.DeviceIdType.MESH
ROWS = 256
HEADS = 8
HEAD = 128
TILES = 8
TOKENS = ROWS // TILES
COLS = TOKENS * HEADS
WINDOW = 20
LAST = WINDOW // 4
KROWS = ROWS + 16
NEG = -1e30
SCALE = math.log2(math.e) / math.sqrt(HEAD)


def attend(slot, first, kbuf, vbuf, qt, onehot, top, total, acc):
    keys = kbuf[slot, :ROWS, :]
    values = vbuf[slot]
    below = kbuf[slot, ROWS:, :].astype(jnp.float32)[:8]
    below = jnp.concatenate([below, below], axis=1)
    at = lax.broadcasted_iota(jnp.int32, (ROWS, COLS), 0).astype(jnp.float32)
    for j in range(TILES):
        scores = jnp.dot(keys, qt[j], preferred_element_type=jnp.float32) * SCALE
        begin = jnp.sum(onehot[j] * below, axis=0, keepdims=True)
        allowed = at >= begin
        if first:
            own = lax.broadcasted_iota(jnp.int32, (1, COLS), 1) // HEADS + j * TOKENS
            allowed = allowed & (at <= own.astype(jnp.float32))
        scores = jnp.where(allowed, scores, NEG)
        high = jnp.max(scores, axis=0, keepdims=True)
        if not first:
            high = jnp.maximum(top[j], high)
        weights = jnp.exp2(scores - high)
        part = jnp.sum(weights.reshape(ROWS // 8, 8, COLS), axis=0)
        mixed = jnp.dot(values, weights.astype(jnp.bfloat16), preferred_element_type=jnp.float32)
        if first:
            total[j] = part
            acc[j] = mixed
        else:
            factor = jnp.exp2(top[j] - high)
            total[j] = total[j] * factor + part
            acc[j] = acc[j] * factor + mixed
        top[j] = high


def kernel(q_ref, k_ref, v_ref, seg_ref, out_ref, kbuf, vbuf, qt, onehot, top, total, acc, turned, stage,
           recv_k, recv_v, send_k, send_v, out_send, out_recv):
    r = lax.axis_index("ctx")
    t = lax.axis_index("tp")
    z, y = r // 4, r % 4
    right = jnp.where(y < 3, r + 1, r - 3)
    left = jnp.where(y > 0, r - 1, r + 3)
    up = jnp.where(z < 7, r + 4, r - 28)
    down = jnp.where(z > 0, r - 4, r + 28)
    to_right = right - r
    to_left = left - r
    reach = jnp.minimum(r, WINDOW)

    barrier = pltpu.get_barrier_semaphore()
    for other in (right, left, up, down):
        pl.semaphore_signal(barrier, inc=1, device_id=(other, t), device_id_type=MESH)
    for step in range(1, TILES):
        pl.semaphore_signal(barrier, inc=1, device_id=(r, lax.rem(t + step, TILES)), device_id_type=MESH)

    seg = seg_ref[...]
    ids = lax.broadcasted_iota(jnp.int32, (8, ROWS), 0)
    counts = jnp.sum((seg < ids).astype(jnp.float32), axis=1, keepdims=True)
    counts = jnp.broadcast_to(counts, (8, HEAD))
    kbuf[0, :ROWS, :] = k_ref[...]
    kbuf[0, ROWS:, :] = jnp.concatenate([counts, counts], axis=0).astype(jnp.bfloat16)
    vbuf[0] = v_ref[...].T

    document = (seg == ids).astype(jnp.bfloat16)
    for j in range(TILES):
        qt[j] = q_ref[pl.ds(j * COLS, COLS), :].T
        token = lax.broadcasted_iota(jnp.int32, (ROWS, COLS), 0)
        column = lax.broadcasted_iota(jnp.int32, (ROWS, COLS), 1)
        spread = jnp.where(token == column // HEADS + j * TOKENS, 1.0, 0.0).astype(jnp.bfloat16)
        onehot[j] = jnp.dot(document, spread, preferred_element_type=jnp.float32)

    pl.semaphore_wait(barrier, 4 + TILES - 1)

    def moved_k(src, dst, to, way, d):
        return pltpu.make_async_remote_copy(
            src_ref=kbuf.at[src], dst_ref=kbuf.at[dst], send_sem=send_k.at[way, d], recv_sem=recv_k.at[dst],
            device_id=(to, t), device_id_type=MESH)

    def moved_v(src, dst, to, way, d):
        return pltpu.make_async_remote_copy(
            src_ref=vbuf.at[src], dst_ref=vbuf.at[dst], send_sem=send_v.at[way, d], recv_sem=recv_v.at[dst],
            device_id=(to, t), device_id_type=MESH)

    def inside(slot):
        return (slot >= 1) & (slot <= WINDOW)

    def held(slot):
        return (slot >= 1) & (slot <= reach)

    def clipped(slot):
        return jnp.clip(slot, 0, WINDOW)

    def own_moves(d, move, act):
        slot = 4 * d
        have = slot <= reach

        @pl.when(have & (z < 7) & (d < LAST))
        def _():
            act(move(slot, clipped(slot + 4), up, 0, d))

        @pl.when(have & inside(slot + to_right))
        def _():
            act(move(slot, clipped(slot + to_right), right, 1, d))

        @pl.when(have & inside(slot + to_left))
        def _():
            act(move(slot, clipped(slot + to_left), left, 2, d))

    def relay(slot, shift, to, way, d, move, act, also):
        @pl.when(held(slot) & inside(slot + shift) & also)
        def _():
            act(move(clipped(slot), clipped(slot + shift), to, way, d))

    def from_left(d):
        return 4 * d - to_left

    def from_right(d):
        return 4 * d - to_right

    def across(d):
        return jnp.where(y >= 2, 4 * d + 2, 4 * d - 2)

    def left_relays_k(d, act):
        relay(from_left(d), to_right, right, 3, d, moved_k, act, True)

    def left_relays_v(d, act):
        relay(from_left(d), to_right, right, 3, d, moved_v, act, (d == 0) & (y == 2))

    def right_relays_v(d, act):
        relay(from_right(d), to_left, left, 4, d, moved_v, act, (d > 0) | (y != 0))

    def right_relays_k(d, act):
        relay(from_right(d), to_left, left, 4, d, moved_k, act, (d == LAST) & (y == 1))

    def start(copy):
        copy.start()

    def wait_k(slot):
        moved_k(slot, slot, right, 0, 0).wait_recv()

    def wait_v(slot):
        moved_v(slot, slot, right, 0, 0).wait_recv()

    own_moves(0, moved_k, start)
    own_moves(0, moved_v, start)
    attend(0, True, kbuf, vbuf, qt, onehot, top, total, acc)

    def one(i, carry):
        d, place = i // 4, i % 4
        l_slot, r_slot, a_slot = from_left(d), from_right(d), across(d)
        slot = jnp.where(place == 0, l_slot, jnp.where(place == 1, r_slot, jnp.where(place == 2, 4 * d + 4, a_slot)))
        have = held(slot)
        slot = clipped(slot)

        @pl.when((place == 0) & (d < LAST) & (4 * d + 4 <= reach))
        def _():
            wait_k(4 * d + 4)
            own_moves(d + 1, moved_k, start)
            wait_v(4 * d + 4)
            own_moves(d + 1, moved_v, start)

        @pl.when(have & (place != 2))
        def _():
            wait_k(slot)

            @pl.when(place == 0)
            def _():
                left_relays_k(d, start)

            @pl.when(place == 1)
            def _():
                right_relays_k(d, start)

            wait_v(slot)

            @pl.when(place == 0)
            def _():
                left_relays_v(d, start)

            @pl.when(place == 1)
            def _():
                right_relays_v(d, start)

        @pl.when(have)
        def _():
            attend(slot, False, kbuf, vbuf, qt, onehot, top, total, acc)

        return carry

    lax.fori_loop(0, 4 * (LAST + 1), one, 0)

    def out_copy(j):
        return pltpu.make_async_remote_copy(
            src_ref=stage.at[j], dst_ref=out_ref.at[:, pl.ds(pl.multiple_of(t * COLS * 4, COLS * 4), COLS * 4)],
            send_sem=out_send.at[j], recv_sem=out_recv.at[t], device_id=(r, j), device_id_type=MESH)

    def finish(step, carry):
        j = lax.rem(t + 1 + step, TILES)
        whole = acc[j] / jnp.sum(total[j], axis=0, keepdims=True)
        turned[...] = whole.T
        for h in range(HEADS):
            stage[j, :, h * HEAD:(h + 1) * HEAD] = turned[pl.ds(h, TOKENS, stride=HEADS), :].astype(jnp.bfloat16)

        @pl.when(step > 0)
        def _():
            out_copy(lax.rem(t + step, TILES)).start()

        return carry

    lax.fori_loop(0, TILES, finish, 0)
    out_ref[:, pl.ds(pl.multiple_of(t * COLS * 4, COLS * 4), COLS * 4)] = stage[t]

    def settle(d, carry):
        def done(copy):
            copy.wait_send()

        own_moves(d, moved_k, done)
        own_moves(d, moved_v, done)
        left_relays_k(d, done)
        left_relays_v(d, done)
        right_relays_v(d, done)
        right_relays_k(d, done)
        return carry

    lax.fori_loop(0, LAST + 1, settle, 0)

    def landed(step, carry):
        j = lax.rem(t + step, TILES)
        out_copy(j).wait_send()
        pltpu.make_async_remote_copy(
            src_ref=stage.at[j],
            dst_ref=out_ref.at[:, pl.ds(pl.multiple_of(j * COLS * 4, COLS * 4), COLS * 4)],
            send_sem=out_send.at[j], recv_sem=out_recv.at[j], device_id=(r, j), device_id_type=MESH).wait_recv()
        return carry

    lax.fori_loop(1, TILES, landed, 0)


def local(queries, keys, values, segment_ids):
    rows, heads, head = queries.shape
    vmem = pl.BlockSpec(memory_space=pltpu.VMEM)
    return pl.pallas_call(
        kernel,
        out_shape=jax.ShapeDtypeStruct((TOKENS, TILES * heads * head), jnp.bfloat16),
        in_specs=[vmem] * 4,
        out_specs=vmem,
        scratch_shapes=[
            pltpu.VMEM((WINDOW + 1, KROWS, HEAD), jnp.bfloat16),
            pltpu.VMEM((WINDOW + 1, HEAD, ROWS), jnp.bfloat16),
            pltpu.VMEM((TILES, HEAD, COLS), jnp.bfloat16),
            pltpu.VMEM((TILES, 8, COLS), jnp.float32),
            pltpu.VMEM((TILES, 1, COLS), jnp.float32),
            pltpu.VMEM((TILES, 8, COLS), jnp.float32),
            pltpu.VMEM((TILES, HEAD, COLS), jnp.float32),
            pltpu.VMEM((COLS, HEAD), jnp.float32),
            pltpu.VMEM((TILES, TOKENS, HEADS * HEAD), jnp.bfloat16),
            pltpu.SemaphoreType.DMA((WINDOW + 1,)),
            pltpu.SemaphoreType.DMA((WINDOW + 1,)),
            pltpu.SemaphoreType.DMA((5, LAST + 1)),
            pltpu.SemaphoreType.DMA((5, LAST + 1)),
            pltpu.SemaphoreType.DMA((TILES,)),
            pltpu.SemaphoreType.DMA((TILES,)),
        ],
        compiler_params=pltpu.CompilerParams(collective_id=0, has_side_effects=True),
    )(queries.reshape(rows * heads, head), keys.reshape(rows, head), values.reshape(rows, head),
      segment_ids.reshape(1, rows))


def solution(mesh):
    in_specs = (P("ctx", "tp", None), P("ctx", "tp", None), P("ctx", "tp", None), P("ctx"))
    out_specs = P(("ctx", "tp"), None)
    return jax.shard_map(local, mesh=mesh, in_specs=in_specs, out_specs=out_specs, check_vma=False)
```

```python
import functools
import math

import jax
import jax.numpy as jnp
from jax import lax
from jax.experimental import pallas as pl
from jax.experimental.pallas import tpu as pltpu
from jax.sharding import PartitionSpec as P

MESH = pl.DeviceIdType.MESH
ROWS = 256
HEADS = 8
HEAD = 128
DOCS = 8
TILES = 8
TOKENS = ROWS // TILES
COLS = TOKENS * HEADS
WINDOW = 20
LAST = WINDOW // 4
KROWS = ROWS + 16
AHEAD = 3
SLOTS = 4
NEG = -1e30
SCALE = math.log2(math.e) / math.sqrt(HEAD)


def attend(blocks, first, kbuf, vbuf, qt, top, acc, held_scores):
    at = lax.broadcasted_iota(jnp.int32, (ROWS, HEAD), 0).astype(jnp.float32)
    keys, values = [], []
    for slot, counts_too in blocks:
        below = kbuf[slot, ROWS:, :].astype(jnp.float32)[:1]
        if counts_too is not True:
            below = jnp.where(counts_too, below, float(ROWS))
        before = jnp.where(at < below, 1.0, 0.0).astype(jnp.bfloat16)
        keys.append(jnp.concatenate([kbuf[slot, :ROWS, :], before], axis=1))
        values.append(vbuf[slot])
    rows = ROWS * len(blocks)
    keys = jnp.concatenate(keys, axis=0) if len(blocks) > 1 else keys[0]
    values = jnp.concatenate(values, axis=1) if len(blocks) > 1 else values[0]

    values = jnp.concatenate([values, jnp.ones((16, rows), jnp.bfloat16)], axis=0)

    def scored(j):
        scores = jnp.dot(keys, qt[j], preferred_element_type=jnp.float32)
        if first:
            key = lax.broadcasted_iota(jnp.int32, (ROWS, COLS), 0)
            own = lax.broadcasted_iota(jnp.int32, (1, COLS), 1) // HEADS + j * TOKENS
            scores = jnp.where(key <= own, scores, NEG)
        held_scores[j % SLOTS, :rows] = scores
        return jnp.max(scores, axis=0, keepdims=True) * SCALE

    def add(j, mixed, factor):
        mixed = mixed[:HEAD + 8]
        acc[j] = mixed if first else acc[j] * factor + mixed

    ahead = [scored(j) for j in range(AHEAD)]
    waiting = None
    for j in range(TILES):
        high = ahead.pop(0)
        if j + AHEAD < TILES:
            ahead.append(scored(j + AHEAD))
        factor = None
        if not first:
            high = jnp.maximum(top[j], high)
            factor = jnp.exp2(top[j] - high)
        weights = jnp.exp2(held_scores[j % SLOTS, :rows] * SCALE - high)
        mixed = jnp.dot(values, weights.astype(jnp.bfloat16), preferred_element_type=jnp.float32)
        top[j] = high
        if waiting is not None:
            add(*waiting)
        waiting = (j, mixed, factor)
    add(*waiting)


def kernel(q_ref, k_ref, v_ref, seg_ref, out_ref, kbuf, vbuf, qt, top, acc, held_scores, turned, stage,
           recv_k, recv_v, send_k, send_v, out_send, out_recv):
    r = lax.axis_index("ctx")
    t = lax.axis_index("tp")
    z, y = r // 4, r % 4
    right = jnp.where(y < 3, r + 1, r - 3)
    left = jnp.where(y > 0, r - 1, r + 3)
    up = jnp.where(z < 7, r + 4, r - 28)
    down = jnp.where(z > 0, r - 4, r + 28)
    to_right = right - r
    to_left = left - r
    reach = jnp.minimum(r, WINDOW)

    barrier = pltpu.get_barrier_semaphore()
    for other in (right, left, up, down):
        pl.semaphore_signal(barrier, inc=1, device_id=(other, t), device_id_type=MESH)
    for step in range(1, TILES):
        pl.semaphore_signal(barrier, inc=1, device_id=(r, lax.rem(t + step, TILES)), device_id_type=MESH)

    seg = seg_ref[...]
    ids = lax.broadcasted_iota(jnp.int32, (HEAD, ROWS), 0)
    smaller = jnp.where((seg < ids) & (ids < DOCS), 1.0, 0.0).astype(jnp.bfloat16)
    counts = lax.dot_general(jnp.ones((16, ROWS), jnp.bfloat16), smaller, (((1,), (1,)), ((), ())),
                             preferred_element_type=jnp.float32)
    kbuf[0, :ROWS, :] = k_ref[...]
    kbuf[0, ROWS:, :] = counts.astype(jnp.bfloat16)
    vbuf[0] = v_ref[...].T

    document = jnp.where(seg == ids, NEG, 0.0).astype(jnp.bfloat16)
    for j in range(TILES):
        qt[j, :HEAD] = q_ref[pl.ds(j * COLS, COLS), :].T
        token = lax.broadcasted_iota(jnp.int32, (ROWS, COLS), 0)
        column = lax.broadcasted_iota(jnp.int32, (ROWS, COLS), 1)
        spread = jnp.where(token == column // HEADS + j * TOKENS, 1.0, 0.0).astype(jnp.bfloat16)
        qt[j, HEAD:] = jnp.dot(document, spread, preferred_element_type=jnp.float32).astype(jnp.bfloat16)

    pl.semaphore_wait(barrier, 4 + TILES - 1)

    def moved_k(src, dst, to, way, d):
        return pltpu.make_async_remote_copy(
            src_ref=kbuf.at[src], dst_ref=kbuf.at[dst], send_sem=send_k.at[way, d], recv_sem=recv_k.at[dst],
            device_id=(to, t), device_id_type=MESH)

    def moved_v(src, dst, to, way, d):
        return pltpu.make_async_remote_copy(
            src_ref=vbuf.at[src], dst_ref=vbuf.at[dst], send_sem=send_v.at[way, d], recv_sem=recv_v.at[dst],
            device_id=(to, t), device_id_type=MESH)

    def inside(slot):
        return (slot >= 1) & (slot <= WINDOW)

    def held(slot):
        return (slot >= 1) & (slot <= reach)

    def clipped(slot):
        return jnp.clip(slot, 0, WINDOW)

    def own_moves(d, move, act):
        slot = 4 * d
        have = slot <= reach

        @pl.when(have & (z < 7) & (d < LAST))
        def _():
            act(move(slot, clipped(slot + 4), up, 0, d))

        @pl.when(have & inside(slot + to_right))
        def _():
            act(move(slot, clipped(slot + to_right), right, 1, d))

        @pl.when(have & inside(slot + to_left))
        def _():
            act(move(slot, clipped(slot + to_left), left, 2, d))

    def relay(slot, shift, to, way, d, move, act, also):
        @pl.when(held(slot) & inside(slot + shift) & also)
        def _():
            act(move(clipped(slot), clipped(slot + shift), to, way, d))

    def from_left(d):
        return 4 * d - to_left

    def from_right(d):
        return 4 * d - to_right

    def across(d):
        return jnp.where(y >= 2, 4 * d + 2, 4 * d - 2)

    def left_relays_k(d, act):
        relay(from_left(d), to_right, right, 3, d, moved_k, act, True)

    def left_relays_v(d, act):
        relay(from_left(d), to_right, right, 3, d, moved_v, act, (d == 0) & (y == 2))

    def right_relays_v(d, act):
        relay(from_right(d), to_left, left, 4, d, moved_v, act, (d > 0) | (y != 0))

    def right_relays_k(d, act):
        relay(from_right(d), to_left, left, 4, d, moved_k, act, (d == LAST) & (y == 1))

    def start(copy):
        copy.start()

    def wait_k(slot):
        moved_k(slot, slot, right, 0, 0).wait_recv()

    def wait_v(slot):
        moved_v(slot, slot, right, 0, 0).wait_recv()

    own_moves(0, moved_k, start)
    own_moves(0, moved_v, start)
    attend([(0, True)], True, kbuf, vbuf, qt, top, acc, held_scores)

    def turn(p):
        y0 = jnp.where(p == 0, 2, jnp.where(p == 19, 23, p + 3))
        y1 = jnp.where(p == 0, 0, jnp.where(p == 18, 21, jnp.where(p == 19, 23, jnp.where(p == 1, 2, p + 2))))
        y2 = jnp.where(p == 0, 0, jnp.where(p == 19, 21, p + 1))
        return jnp.where(y == 0, y0, jnp.where(y == 1, y1, jnp.where(y == 2, y2, p)))

    def serve(p):
        i = turn(p)
        d, place = i // 4, i % 4
        slot = jnp.where(place == 0, from_left(d), jnp.where(place == 1, from_right(d), jnp.where(
            place == 2, 4 * d + 4, across(d))))
        have = held(slot)
        slot = clipped(slot)

        @pl.when(have)
        def _():
            wait_k(slot)

            @pl.when(place == 0)
            def _():
                left_relays_k(d, start)

            @pl.when(place == 1)
            def _():
                right_relays_k(d, start)

            @pl.when(place == 2)
            def _():
                own_moves(d + 1, moved_k, start)

            wait_v(slot)

            @pl.when(place == 0)
            def _():
                left_relays_v(d, start)

            @pl.when(place == 1)
            def _():
                right_relays_v(d, start)

            @pl.when(place == 2)
            def _():
                own_moves(d + 1, moved_v, start)

        return jnp.where(have, slot, 0), have

    def one(n, carry):
        slot_a, have_a = serve(2 * n)
        slot_b, have_b = serve(2 * n + 1)

        @pl.when(have_a | have_b)
        def _():
            attend([(slot_a, have_a), (slot_b, have_b)], False, kbuf, vbuf, qt, top, acc, held_scores)

        return carry

    lax.fori_loop(0, WINDOW // 2, one, 0)

    def out_copy(j):
        return pltpu.make_async_remote_copy(
            src_ref=stage.at[j], dst_ref=out_ref.at[:, pl.ds(pl.multiple_of(t * COLS * 4, COLS * 4), COLS * 4)],
            send_sem=out_send.at[j], recv_sem=out_recv.at[t], device_id=(r, j), device_id_type=MESH)

    def finish(step, carry):
        j = lax.rem(t + 1 + step, TILES)
        whole = acc[j, :HEAD] / acc[j, HEAD:HEAD + 1]
        turned[...] = whole.T
        for h in range(HEADS):
            stage[j, :, h * HEAD:(h + 1) * HEAD] = turned[pl.ds(h, TOKENS, stride=HEADS), :].astype(jnp.bfloat16)

        @pl.when(step > 0)
        def _():
            out_copy(lax.rem(t + step, TILES)).start()

        return carry

    lax.fori_loop(0, TILES, finish, 0)
    out_ref[:, pl.ds(pl.multiple_of(t * COLS * 4, COLS * 4), COLS * 4)] = stage[t]

    def settle(d, carry):
        def done(copy):
            copy.wait_send()

        own_moves(d, moved_k, done)
        own_moves(d, moved_v, done)
        left_relays_k(d, done)
        left_relays_v(d, done)
        right_relays_v(d, done)
        right_relays_k(d, done)
        return carry

    lax.fori_loop(0, LAST + 1, settle, 0)

    def landed(step, carry):
        j = lax.rem(t + step, TILES)
        out_copy(j).wait_send()
        pltpu.make_async_remote_copy(
            src_ref=stage.at[j],
            dst_ref=out_ref.at[:, pl.ds(pl.multiple_of(j * COLS * 4, COLS * 4), COLS * 4)],
            send_sem=out_send.at[j], recv_sem=out_recv.at[j], device_id=(r, j), device_id_type=MESH).wait_recv()
        return carry

    lax.fori_loop(1, TILES, landed, 0)


def local(queries, keys, values, segment_ids):
    rows, heads, head = queries.shape
    vmem = pl.BlockSpec(memory_space=pltpu.VMEM)
    return pl.pallas_call(
        kernel,
        out_shape=jax.ShapeDtypeStruct((TOKENS, TILES * heads * head), jnp.bfloat16),
        in_specs=[vmem] * 4,
        out_specs=vmem,
        scratch_shapes=[
            pltpu.VMEM((WINDOW + 1, KROWS, HEAD), jnp.bfloat16),
            pltpu.VMEM((WINDOW + 1, HEAD, ROWS), jnp.bfloat16),
            pltpu.VMEM((TILES, 2 * HEAD, COLS), jnp.bfloat16),
            pltpu.VMEM((TILES, 1, COLS), jnp.float32),
            pltpu.VMEM((TILES, HEAD + 8, COLS), jnp.float32),
            pltpu.VMEM((SLOTS, 2 * ROWS, COLS), jnp.float32),
            pltpu.VMEM((COLS, HEAD), jnp.float32),
            pltpu.VMEM((TILES, TOKENS, HEADS * HEAD), jnp.bfloat16),
            pltpu.SemaphoreType.DMA((WINDOW + 1,)),
            pltpu.SemaphoreType.DMA((WINDOW + 1,)),
            pltpu.SemaphoreType.DMA((5, LAST + 1)),
            pltpu.SemaphoreType.DMA((5, LAST + 1)),
            pltpu.SemaphoreType.DMA((TILES,)),
            pltpu.SemaphoreType.DMA((TILES,)),
        ],
        compiler_params=pltpu.CompilerParams(collective_id=0, has_side_effects=True),
    )(queries.reshape(rows * heads, head), keys.reshape(rows, head), values.reshape(rows, head),
      segment_ids.reshape(1, rows))


def solution(mesh):
    in_specs = (P("ctx", "tp", None), P("ctx", "tp", None), P("ctx", "tp", None), P("ctx"))
    out_specs = P(("ctx", "tp"), None)
    return jax.shard_map(local, mesh=mesh, in_specs=in_specs, out_specs=out_specs, check_vma=False)
```

```python
import functools
import math

import jax
import jax.numpy as jnp
from jax import lax
from jax.experimental import pallas as pl
from jax.experimental.pallas import tpu as pltpu
from jax.sharding import PartitionSpec as P

MESH = pl.DeviceIdType.MESH
ROWS = 256
HEADS = 8
HEAD = 128
DOCS = 8
TILES = 8
TOKENS = ROWS // TILES
COLS = TOKENS * HEADS
CTX = 32
WINDOW = 20
LAST = WINDOW // 4
KROWS = ROWS + 16
PIECES = ((0, 128), (128, 144)), ((0, 64), (64, 64))
AHEAD = 3
SLOTS = 4
LEFT_K, RIGHT_K = (2,), (18,)
LEFT_V, RIGHT_V = (6, 10, 14), (2, 18)
ACROSS_K, ACROSS_V = (6, 10, 14), ()
NEG = -1e30
SCALE = math.log2(math.e) / math.sqrt(HEAD)


def order_of(column):
    listed = []
    for name in ARRIVAL.split():
        place, d = "LRoX".index(name[0]), int(name[1])
        slot = 4 * d + (column - (column + (-1, 1, 0, 2)[place]) % 4)
        if 1 <= slot <= WINDOW:
            listed.append(4 * d + place)
    return listed


ARRIVAL = (
    "o1 L0 R0 o2 "
    "L1 R1 X0 o3 "
    "L2 R2 X1 o4 "
    "L3 R3 X2 o5 "
    "L4 R4 X3 L5 "
    "R5 X4 X5 "
)
ORDER = [order_of(column) for column in range(4)]


def attend(blocks, first, kbuf, vbuf, qt, top, acc, held_scores):
    at = lax.broadcasted_iota(jnp.int32, (ROWS, HEAD), 0).astype(jnp.float32)
    keys, values = [], []
    for slot, counts_too in blocks:
        below = kbuf[slot, ROWS:, :].astype(jnp.float32)[:1]
        if counts_too is not True:
            below = jnp.where(counts_too, below, float(ROWS))
        before = jnp.where(at < below, 1.0, 0.0).astype(jnp.bfloat16)
        keys.append(jnp.concatenate([kbuf[slot, :ROWS, :], before], axis=1))
        values.append(vbuf[slot])
    rows = ROWS * len(blocks)
    keys = jnp.concatenate(keys, axis=0) if len(blocks) > 1 else keys[0]
    values = jnp.concatenate(values, axis=1) if len(blocks) > 1 else values[0]

    values = jnp.concatenate([values, jnp.ones((16, rows), jnp.bfloat16)], axis=0)

    def scored(j):
        scores = jnp.dot(keys, qt[j], preferred_element_type=jnp.float32)
        if first:
            key = lax.broadcasted_iota(jnp.int32, (ROWS, COLS), 0)
            own = lax.broadcasted_iota(jnp.int32, (1, COLS), 1) // HEADS + j * TOKENS
            scores = jnp.where(key <= own, scores, NEG)
        held_scores[j % SLOTS, :rows] = scores
        return jnp.max(scores, axis=0, keepdims=True) * SCALE

    def add(j, mixed, factor):
        mixed = mixed[:HEAD + 8]
        acc[j] = mixed if first else acc[j] * factor + mixed

    ahead = [scored(j) for j in range(AHEAD)]
    waiting = None
    for j in range(TILES):
        high = ahead.pop(0)
        if j + AHEAD < TILES:
            ahead.append(scored(j + AHEAD))
        factor = None
        if not first:
            high = jnp.maximum(top[j], high)
            factor = jnp.exp2(top[j] - high)
        weights = jnp.exp2(held_scores[j % SLOTS, :rows] * SCALE - high)
        mixed = jnp.dot(values, weights.astype(jnp.bfloat16), preferred_element_type=jnp.float32)
        top[j] = high
        if waiting is not None:
            add(*waiting)
        waiting = (j, mixed, factor)
    add(*waiting)


def kernel(q_ref, k_ref, v_ref, seg_ref, out_ref, kbuf, vbuf, qt, top, acc, held_scores, turned, stage,
           recv_k, recv_v, send_k, send_v, out_send, out_recv):
    r = lax.axis_index("ctx")
    t = lax.axis_index("tp")
    z, y = r // 4, r % 4
    right = jnp.where(y < 3, r + 1, r - 3)
    left = jnp.where(y > 0, r - 1, r + 3)
    up = jnp.where(z < 7, r + 4, r - 28)
    down = jnp.where(z > 0, r - 4, r + 28)
    to_right = right - r
    to_left = left - r
    reach = jnp.minimum(r, WINDOW)

    barrier = pltpu.get_barrier_semaphore()
    for other in (right, left, up, down, lax.rem(r + 4 * LAST, CTX), lax.rem(r + CTX - 4 * LAST, CTX)):
        pl.semaphore_signal(barrier, inc=1, device_id=(other, t), device_id_type=MESH)
    for step in range(1, TILES):
        pl.semaphore_signal(barrier, inc=1, device_id=(r, lax.rem(t + step, TILES)), device_id_type=MESH)

    seg = seg_ref[...]
    ids = lax.broadcasted_iota(jnp.int32, (HEAD, ROWS), 0)
    smaller = jnp.where((seg < ids) & (ids < DOCS), 1.0, 0.0).astype(jnp.bfloat16)
    counts = lax.dot_general(jnp.ones((16, ROWS), jnp.bfloat16), smaller, (((1,), (1,)), ((), ())),
                             preferred_element_type=jnp.float32)
    kbuf[0, :ROWS, :] = k_ref[...]
    kbuf[0, ROWS:, :] = counts.astype(jnp.bfloat16)
    vbuf[0] = v_ref[...].T

    document = jnp.where(seg == ids, NEG, 0.0).astype(jnp.bfloat16)
    for j in range(TILES):
        qt[j, :HEAD] = q_ref[pl.ds(j * COLS, COLS), :].T
        token = lax.broadcasted_iota(jnp.int32, (ROWS, COLS), 0)
        column = lax.broadcasted_iota(jnp.int32, (ROWS, COLS), 1)
        spread = jnp.where(token == column // HEADS + j * TOKENS, 1.0, 0.0).astype(jnp.bfloat16)
        qt[j, HEAD:] = jnp.dot(document, spread, preferred_element_type=jnp.float32).astype(jnp.bfloat16)

    pl.semaphore_wait(barrier, 6 + TILES - 1)

    def moved(part, piece):
        first, size = PIECES[part][piece] if piece is not None else (0, (KROWS, HEAD)[part])
        buffer, sent, landed_at = ((kbuf, send_k, recv_k), (vbuf, send_v, recv_v))[part]

        def copy(src, dst, to, way, d):
            return pltpu.make_async_remote_copy(
                src_ref=buffer.at[src, pl.ds(first, size)], dst_ref=buffer.at[dst, pl.ds(first, size)],
                send_sem=sent.at[way, d], recv_sem=landed_at.at[piece or 0, dst],
                device_id=(to, t), device_id_type=MESH)

        return copy

    def sender(part, piece):
        return lambda *where: moved(part, piece)(*where).start()

    def waiter(part):
        return lambda *where: moved(part, None)(*where).wait_send()

    def inside(slot):
        return (slot >= 1) & (slot <= WINDOW)

    def held(slot):
        return (slot >= 1) & (slot <= reach)

    def clipped(slot):
        return jnp.clip(slot, 0, WINDOW)

    def own_moves(d, act):
        slot = 4 * d
        have = slot <= reach

        @pl.when(have & (z < 7) & (d < LAST - 1))
        def _():
            act(slot, clipped(slot + 4), up, 0, d)

        @pl.when(have & inside(slot + to_right))
        def _():
            act(slot, clipped(slot + to_right), right, 1, d)

        @pl.when(have & inside(slot + to_left))
        def _():
            act(slot, clipped(slot + to_left), left, 2, d)

    def far_moves(act):
        @pl.when(z + LAST <= 7)
        def _():
            act(0, WINDOW, r + 4 * LAST, 5, 0)

    def across_moves(part, d, act):
        slot = across(d)

        @pl.when(held(slot) & (z < 7) & any_of(slot + 4, (ACROSS_K, ACROSS_V)[part]))
        def _():
            act(clipped(slot), clipped(slot + 4), up, 6, d)

    def relay(slot, shift, to, way, d, act, also):
        @pl.when(held(slot) & inside(slot + shift) & also)
        def _():
            act(clipped(slot), clipped(slot + shift), to, way, d)

    def from_left(d):
        return 4 * d - to_left

    def from_right(d):
        return 4 * d - to_right

    def across(d):
        return jnp.where(y >= 2, 4 * d + 2, 4 * d - 2)

    def any_of(slot, slots):
        found = slot < 0
        for other in slots:
            found = found | (slot == other)
        return found

    def left_relays(part, d, act):
        to = from_left(d) + to_right
        also = any_of(to, (LEFT_K, LEFT_V)[part])
        if part == 1:
            also = also | ((to == 2) & (y == 2))
        relay(from_left(d), to_right, right, 3, d, act, also)

    def right_relays(part, d, act):
        relay(from_right(d), to_left, left, 4, d, act, any_of(from_right(d) + to_left, (RIGHT_K, RIGHT_V)[part]))

    def await_piece(part, piece, slot):
        moved(part, piece)(slot, slot, right, 0, 0).wait_recv()

    for part in range(2):
        for piece in range(2):
            own_moves(0, sender(part, piece))
    for part in range(2):
        for piece in range(2):
            far_moves(sender(part, piece))
    attend([(0, True)], True, kbuf, vbuf, qt, top, acc, held_scores)

    def turn(n):
        pairs = [jnp.int32(0)] * 4
        for column in range(4):
            orders = ORDER[column]
            for m in range(WINDOW // 2):
                pairs[column] = jnp.where(n == m, 32 * orders[2 * m] + orders[2 * m + 1], pairs[column])
        pair = jnp.where(y == 0, pairs[0], jnp.where(y == 1, pairs[1], jnp.where(y == 2, pairs[2], pairs[3])))
        return pair // 32, pair % 32

    def serve(i):
        d, place = i // 4, i % 4
        slot = jnp.where(place == 0, from_left(d), jnp.where(place == 1, from_right(d), jnp.where(
            place == 2, 4 * d, across(d))))
        have = held(slot)
        slot = clipped(slot)

        for at in range(4):
            @pl.when(have & (place == at))
            def _():
                for part in range(2):
                    for piece in range(2):
                        await_piece(part, piece, slot)
                        act = sender(part, piece)
                        if at == 0:
                            left_relays(part, d, act)
                        elif at == 1:
                            right_relays(part, d, act)
                        elif at == 2:
                            own_moves(d, act)
                        else:
                            across_moves(part, d, act)

        return jnp.where(have, slot, 0), have

    def one(n, carry):
        a, b = turn(n)
        slot_a, have_a = serve(a)
        slot_b, have_b = serve(b)

        @pl.when(have_a | have_b)
        def _():
            attend([(slot_a, have_a), (slot_b, have_b)], False, kbuf, vbuf, qt, top, acc, held_scores)

        return carry

    lax.fori_loop(0, WINDOW // 2, one, 0)

    def out_copy(j):
        return pltpu.make_async_remote_copy(
            src_ref=stage.at[j], dst_ref=out_ref.at[:, pl.ds(pl.multiple_of(t * COLS * 4, COLS * 4), COLS * 4)],
            send_sem=out_send.at[j], recv_sem=out_recv.at[t], device_id=(r, j), device_id_type=MESH)

    def finish(step, carry):
        j = lax.rem(t + 1 + step, TILES)
        whole = acc[j, :HEAD] / acc[j, HEAD:HEAD + 1]
        turned[...] = whole.T
        for h in range(HEADS):
            stage[j, :, h * HEAD:(h + 1) * HEAD] = turned[pl.ds(h, TOKENS, stride=HEADS), :].astype(jnp.bfloat16)

        @pl.when(step > 0)
        def _():
            out_copy(lax.rem(t + step, TILES)).start()

        return carry

    lax.fori_loop(0, TILES, finish, 0)
    out_ref[:, pl.ds(pl.multiple_of(t * COLS * 4, COLS * 4), COLS * 4)] = stage[t]

    def settle(d, carry):
        for part in range(2):
            own_moves(d, waiter(part))
            across_moves(part, d, waiter(part))
            left_relays(part, d, waiter(part))
            right_relays(part, d, waiter(part))
        return carry

    lax.fori_loop(0, LAST + 1, settle, 0)
    for part in range(2):
        far_moves(waiter(part))

    def landed(step, carry):
        j = lax.rem(t + step, TILES)
        out_copy(j).wait_send()
        pltpu.make_async_remote_copy(
            src_ref=stage.at[j],
            dst_ref=out_ref.at[:, pl.ds(pl.multiple_of(j * COLS * 4, COLS * 4), COLS * 4)],
            send_sem=out_send.at[j], recv_sem=out_recv.at[j], device_id=(r, j), device_id_type=MESH).wait_recv()
        return carry

    lax.fori_loop(1, TILES, landed, 0)


def local(queries, keys, values, segment_ids):
    rows, heads, head = queries.shape
    vmem = pl.BlockSpec(memory_space=pltpu.VMEM)
    return pl.pallas_call(
        kernel,
        out_shape=jax.ShapeDtypeStruct((TOKENS, TILES * heads * head), jnp.bfloat16),
        in_specs=[vmem] * 4,
        out_specs=vmem,
        scratch_shapes=[
            pltpu.VMEM((WINDOW + 1, KROWS, HEAD), jnp.bfloat16),
            pltpu.VMEM((WINDOW + 1, HEAD, ROWS), jnp.bfloat16),
            pltpu.VMEM((TILES, 2 * HEAD, COLS), jnp.bfloat16),
            pltpu.VMEM((TILES, 1, COLS), jnp.float32),
            pltpu.VMEM((TILES, HEAD + 8, COLS), jnp.float32),
            pltpu.VMEM((SLOTS, 2 * ROWS, COLS), jnp.float32),
            pltpu.VMEM((COLS, HEAD), jnp.float32),
            pltpu.VMEM((TILES, TOKENS, HEADS * HEAD), jnp.bfloat16),
            pltpu.SemaphoreType.DMA((2, WINDOW + 1)),
            pltpu.SemaphoreType.DMA((2, WINDOW + 1)),
            pltpu.SemaphoreType.DMA((7, LAST + 1)),
            pltpu.SemaphoreType.DMA((7, LAST + 1)),
            pltpu.SemaphoreType.DMA((TILES,)),
            pltpu.SemaphoreType.DMA((TILES,)),
        ],
        compiler_params=pltpu.CompilerParams(collective_id=0, has_side_effects=True),
    )(queries.reshape(rows * heads, head), keys.reshape(rows, head), values.reshape(rows, head),
      segment_ids.reshape(1, rows))


def solution(mesh):
    in_specs = (P("ctx", "tp", None), P("ctx", "tp", None), P("ctx", "tp", None), P("ctx"))
    out_specs = P(("ctx", "tp"), None)
    return jax.shard_map(local, mesh=mesh, in_specs=in_specs, out_specs=out_specs, check_vma=False)
```

```python
import functools
import math

import jax
import jax.numpy as jnp
from jax import lax
from jax.experimental import pallas as pl
from jax.experimental.pallas import tpu as pltpu
from jax.sharding import PartitionSpec as P

MESH = pl.DeviceIdType.MESH
ROWS = 256
HEADS = 8
HEAD = 128
DOCS = 8
TILES = 8
TOKENS = ROWS // TILES
COLS = TOKENS * HEADS
CTX = 32
WINDOW = 20
LAST = WINDOW // 4
KROWS = ROWS + 16
PIECES = ((0, 128), (128, 144)), ((0, 64), (64, 64))
AHEAD = 3
SLOTS = 4
LEFT_K, RIGHT_K = (2,), (18,)
LEFT_V, RIGHT_V = (6, 10, 14), (2, 18)
ACROSS_K, ACROSS_V = (6, 10, 14), ()
NEG = -1e30
SCALE = math.log2(math.e) / math.sqrt(HEAD)


def order_of(column):
    listed = []
    for name in ARRIVAL:
        place, d = "LRoX".index(name[0]), int(name[1])
        slot = 4 * d + (column - (column + (-1, 1, 0, 2)[place]) % 4)
        if 1 <= slot <= WINDOW:
            listed.append(4 * d + place)
    return listed


ARRIVAL = (
    "o1", "L0", "R0", "o2", "L1", "R1", "X0", "o3",
    "L2", "R2", "X1", "o4", "L3", "R3", "X2", "o5",
    "L4", "R4", "X3", "L5", "R5", "X4", "X5",
)
ORDER = [order_of(column) for column in range(4)]


def attend(blocks, first, kbuf, vbuf, qt, top, acc, held_scores):
    at = lax.broadcasted_iota(jnp.int32, (ROWS, HEAD), 0).astype(jnp.float32)
    keys, values = [], []
    for slot, counts_too in blocks:
        below = kbuf[slot, ROWS:, :].astype(jnp.float32)[:1]
        if counts_too is not True:
            below = jnp.where(counts_too, below, float(ROWS))
        before = jnp.where(at < below, 1.0, 0.0).astype(jnp.bfloat16)
        keys.append(jnp.concatenate([kbuf[slot, :ROWS, :], before], axis=1))
        values.append(vbuf[slot])
    rows = ROWS * len(blocks)
    keys = jnp.concatenate(keys, axis=0) if len(blocks) > 1 else keys[0]
    values = jnp.concatenate(values, axis=1) if len(blocks) > 1 else values[0]

    values = jnp.concatenate([values, jnp.ones((16, rows), jnp.bfloat16)], axis=0)

    def scored(j):
        scores = jnp.dot(keys, qt[j], preferred_element_type=jnp.float32)
        if first:
            key = lax.broadcasted_iota(jnp.int32, (ROWS, COLS), 0)
            own = lax.broadcasted_iota(jnp.int32, (1, COLS), 1) // HEADS + j * TOKENS
            scores = jnp.where(key <= own, scores, NEG)
        held_scores[j % SLOTS, :rows] = scores
        return jnp.max(scores, axis=0, keepdims=True) * SCALE

    def add(j, mixed, factor):
        mixed = mixed[:HEAD + 8]
        acc[j] = mixed if first else acc[j] * factor + mixed

    ahead = [scored(j) for j in range(AHEAD)]
    waiting = None
    for j in range(TILES):
        high = ahead.pop(0)
        if j + AHEAD < TILES:
            ahead.append(scored(j + AHEAD))
        factor = None
        if not first:
            high = jnp.maximum(top[j], high)
            factor = jnp.exp2(top[j] - high)
        weights = jnp.exp2(held_scores[j % SLOTS, :rows] * SCALE - high)
        mixed = jnp.dot(values, weights.astype(jnp.bfloat16), preferred_element_type=jnp.float32)
        top[j] = high
        if waiting is not None:
            add(*waiting)
        waiting = (j, mixed, factor)
    add(*waiting)


def kernel(q_hbm, k_hbm, v_hbm, seg_hbm, out_ref, q_ref, v_ref, seg_ref, in_sem, kbuf, vbuf, qt, top, acc, held_scores, turned, stage,
           recv_k, recv_v, send_k, send_v, out_send, out_recv):
    r = lax.axis_index("ctx")
    t = lax.axis_index("tp")
    z, y = r // 4, r % 4
    right = jnp.where(y < 3, r + 1, r - 3)
    left = jnp.where(y > 0, r - 1, r + 3)
    up = jnp.where(z < 7, r + 4, r - 28)
    down = jnp.where(z > 0, r - 4, r + 28)
    to_right = right - r
    to_left = left - r
    reach = jnp.minimum(r, WINDOW)

    barrier = pltpu.get_barrier_semaphore()
    for other in (right, left, up, down, lax.rem(r + 4 * LAST, CTX), lax.rem(r + CTX - 4 * LAST, CTX)):
        pl.semaphore_signal(barrier, inc=1, device_id=(other, t), device_id_type=MESH)
    for step in range(1, TILES):
        pl.semaphore_signal(barrier, inc=1, device_id=(r, lax.rem(t + step, TILES)), device_id_type=MESH)

    taken = [
        pltpu.make_async_copy(seg_hbm, seg_ref, in_sem.at[0]),
        pltpu.make_async_copy(k_hbm, kbuf.at[0, pl.ds(0, ROWS)], in_sem.at[1]),
        pltpu.make_async_copy(v_hbm, v_ref, in_sem.at[2]),
        pltpu.make_async_copy(q_hbm, q_ref, in_sem.at[3]),
    ]
    for copy in taken:
        copy.start()

    taken[0].wait()
    seg = seg_ref[...]
    ids = lax.broadcasted_iota(jnp.int32, (HEAD, ROWS), 0)
    smaller = jnp.where((seg < ids) & (ids < DOCS), 1.0, 0.0).astype(jnp.bfloat16)
    counts = lax.dot_general(jnp.ones((16, ROWS), jnp.bfloat16), smaller, (((1,), (1,)), ((), ())),
                             preferred_element_type=jnp.float32)
    kbuf[0, ROWS:, :] = counts.astype(jnp.bfloat16)
    taken[2].wait()
    vbuf[0] = v_ref[...].T
    taken[1].wait()

    pl.semaphore_wait(barrier, 6 + TILES - 1)

    def moved(part, piece):
        first, size = PIECES[part][piece] if piece is not None else (0, (KROWS, HEAD)[part])
        buffer, sent, landed_at = ((kbuf, send_k, recv_k), (vbuf, send_v, recv_v))[part]

        def copy(src, dst, to, way, d):
            return pltpu.make_async_remote_copy(
                src_ref=buffer.at[src, pl.ds(first, size)], dst_ref=buffer.at[dst, pl.ds(first, size)],
                send_sem=sent.at[way, d], recv_sem=landed_at.at[piece or 0, dst],
                device_id=(to, t), device_id_type=MESH)

        return copy

    def sender(part, piece):
        return lambda *where: moved(part, piece)(*where).start()

    def waiter(part):
        return lambda *where: moved(part, None)(*where).wait_send()

    def inside(slot):
        return (slot >= 1) & (slot <= WINDOW)

    def held(slot):
        return (slot >= 1) & (slot <= reach)

    def clipped(slot):
        return jnp.clip(slot, 0, WINDOW)

    def own_moves(d, act):
        slot = 4 * d
        have = slot <= reach

        @pl.when(have & (z < 7) & (d < LAST - 1))
        def _():
            act(slot, clipped(slot + 4), up, 0, d)

        @pl.when(have & inside(slot + to_right))
        def _():
            act(slot, clipped(slot + to_right), right, 1, d)

        @pl.when(have & inside(slot + to_left))
        def _():
            act(slot, clipped(slot + to_left), left, 2, d)

    def far_moves(act):
        @pl.when(z + LAST <= 7)
        def _():
            act(0, WINDOW, r + 4 * LAST, 5, 0)

    def across_moves(part, d, act):
        slot = across(d)

        @pl.when(held(slot) & (z < 7) & any_of(slot + 4, (ACROSS_K, ACROSS_V)[part]))
        def _():
            act(clipped(slot), clipped(slot + 4), up, 6, d)

    def relay(slot, shift, to, way, d, act, also):
        @pl.when(held(slot) & inside(slot + shift) & also)
        def _():
            act(clipped(slot), clipped(slot + shift), to, way, d)

    def from_left(d):
        return 4 * d - to_left

    def from_right(d):
        return 4 * d - to_right

    def across(d):
        return jnp.where(y >= 2, 4 * d + 2, 4 * d - 2)

    def any_of(slot, slots):
        found = slot < 0
        for other in slots:
            found = found | (slot == other)
        return found

    def left_relays(part, d, act):
        to = from_left(d) + to_right
        also = any_of(to, (LEFT_K, LEFT_V)[part])
        if part == 1:
            also = also | ((to == 2) & (y == 2))
        relay(from_left(d), to_right, right, 3, d, act, also)

    def right_relays(part, d, act):
        relay(from_right(d), to_left, left, 4, d, act, any_of(from_right(d) + to_left, (RIGHT_K, RIGHT_V)[part]))

    def await_piece(part, piece, slot):
        moved(part, piece)(slot, slot, right, 0, 0).wait_recv()

    for part in range(2):
        for piece in range(2):
            own_moves(0, sender(part, piece))
    for part in range(2):
        for piece in range(2):
            far_moves(sender(part, piece))
    taken[3].wait()
    document = jnp.where(seg == ids, NEG, 0.0).astype(jnp.bfloat16)
    for j in range(TILES):
        qt[j, :HEAD] = q_ref[pl.ds(j * COLS, COLS), :].T
        token = lax.broadcasted_iota(jnp.int32, (ROWS, COLS), 0)
        column = lax.broadcasted_iota(jnp.int32, (ROWS, COLS), 1)
        spread = jnp.where(token == column // HEADS + j * TOKENS, 1.0, 0.0).astype(jnp.bfloat16)
        qt[j, HEAD:] = jnp.dot(document, spread, preferred_element_type=jnp.float32).astype(jnp.bfloat16)

    attend([(0, True)], True, kbuf, vbuf, qt, top, acc, held_scores)

    def turn(n):
        pairs = [jnp.int32(0)] * 4
        for column in range(4):
            orders = ORDER[column]
            for m in range(WINDOW // 2):
                pairs[column] = jnp.where(n == m, 32 * orders[2 * m] + orders[2 * m + 1], pairs[column])
        pair = jnp.where(y == 0, pairs[0], jnp.where(y == 1, pairs[1], jnp.where(y == 2, pairs[2], pairs[3])))
        return pair // 32, pair % 32

    def serve(i):
        d, place = i // 4, i % 4
        slot = jnp.where(place == 0, from_left(d), jnp.where(place == 1, from_right(d), jnp.where(
            place == 2, 4 * d, across(d))))
        have = held(slot)
        slot = clipped(slot)

        for at in range(4):
            @pl.when(have & (place == at))
            def _():
                for part in range(2):
                    for piece in range(2):
                        await_piece(part, piece, slot)
                        act = sender(part, piece)
                        if at == 0:
                            left_relays(part, d, act)
                        elif at == 1:
                            right_relays(part, d, act)
                        elif at == 2:
                            own_moves(d, act)
                        else:
                            across_moves(part, d, act)

        return jnp.where(have, slot, 0), have

    def one(n, carry):
        a, b = turn(n)
        slot_a, have_a = serve(a)
        slot_b, have_b = serve(b)

        @pl.when(have_a | have_b)
        def _():
            attend([(slot_a, have_a), (slot_b, have_b)], False, kbuf, vbuf, qt, top, acc, held_scores)

        return carry

    lax.fori_loop(0, WINDOW // 2, one, 0)

    def out_copy(j):
        return pltpu.make_async_remote_copy(
            src_ref=stage.at[j], dst_ref=out_ref.at[:, pl.ds(pl.multiple_of(t * COLS * 4, COLS * 4), COLS * 4)],
            send_sem=out_send.at[j], recv_sem=out_recv.at[t], device_id=(r, j), device_id_type=MESH)

    def finish(step, carry):
        j = lax.rem(t + 1 + step, TILES)
        whole = acc[j, :HEAD] / acc[j, HEAD:HEAD + 1]
        turned[...] = whole.T
        for h in range(HEADS):
            stage[j, :, h * HEAD:(h + 1) * HEAD] = turned[pl.ds(h, TOKENS, stride=HEADS), :].astype(jnp.bfloat16)

        @pl.when(step > 0)
        def _():
            out_copy(lax.rem(t + step, TILES)).start()

        return carry

    lax.fori_loop(0, TILES, finish, 0)
    out_ref[:, pl.ds(pl.multiple_of(t * COLS * 4, COLS * 4), COLS * 4)] = stage[t]

    def settle(d, carry):
        for part in range(2):
            own_moves(d, waiter(part))
            across_moves(part, d, waiter(part))
            left_relays(part, d, waiter(part))
            right_relays(part, d, waiter(part))
        return carry

    lax.fori_loop(0, LAST + 1, settle, 0)
    for part in range(2):
        far_moves(waiter(part))

    def landed(step, carry):
        j = lax.rem(t + step, TILES)
        out_copy(j).wait_send()
        pltpu.make_async_remote_copy(
            src_ref=stage.at[j],
            dst_ref=out_ref.at[:, pl.ds(pl.multiple_of(j * COLS * 4, COLS * 4), COLS * 4)],
            send_sem=out_send.at[j], recv_sem=out_recv.at[j], device_id=(r, j), device_id_type=MESH).wait_recv()
        return carry

    lax.fori_loop(1, TILES, landed, 0)


def local(queries, keys, values, segment_ids):
    rows, heads, head = queries.shape
    vmem = pl.BlockSpec(memory_space=pltpu.VMEM)
    return pl.pallas_call(
        kernel,
        out_shape=pltpu.VMEM((TOKENS, TILES * heads * head), jnp.bfloat16),
        in_specs=[pl.BlockSpec(memory_space=pl.ANY)] * 4,
        out_specs=vmem,
        scratch_shapes=[
            pltpu.VMEM((COLS * TILES, HEAD), jnp.bfloat16),
            pltpu.VMEM((ROWS, HEAD), jnp.bfloat16),
            pltpu.VMEM((1, ROWS), jnp.int32),
            pltpu.SemaphoreType.DMA((4,)),
            pltpu.VMEM((WINDOW + 1, KROWS, HEAD), jnp.bfloat16),
            pltpu.VMEM((WINDOW + 1, HEAD, ROWS), jnp.bfloat16),
            pltpu.VMEM((TILES, 2 * HEAD, COLS), jnp.bfloat16),
            pltpu.VMEM((TILES, 1, COLS), jnp.float32),
            pltpu.VMEM((TILES, HEAD + 8, COLS), jnp.float32),
            pltpu.VMEM((SLOTS, 2 * ROWS, COLS), jnp.float32),
            pltpu.VMEM((COLS, HEAD), jnp.float32),
            pltpu.VMEM((TILES, TOKENS, HEADS * HEAD), jnp.bfloat16),
            pltpu.SemaphoreType.DMA((2, WINDOW + 1)),
            pltpu.SemaphoreType.DMA((2, WINDOW + 1)),
            pltpu.SemaphoreType.DMA((7, LAST + 1)),
            pltpu.SemaphoreType.DMA((7, LAST + 1)),
            pltpu.SemaphoreType.DMA((TILES,)),
            pltpu.SemaphoreType.DMA((TILES,)),
        ],
        compiler_params=pltpu.CompilerParams(collective_id=0, has_side_effects=True),
    )(queries.reshape(rows * heads, head), keys.reshape(rows, head), values.reshape(rows, head),
      segment_ids.reshape(1, rows))


def solution(mesh):
    in_specs = (P("ctx", "tp", None), P("ctx", "tp", None), P("ctx", "tp", None), P("ctx"))
    out_specs = P(("ctx", "tp"), None)
    return jax.shard_map(local, mesh=mesh, in_specs=in_specs, out_specs=out_specs, check_vma=False)
```

```python
import functools
import math

import jax
import jax.numpy as jnp
from jax import lax
from jax.experimental import pallas as pl
from jax.experimental.pallas import tpu as pltpu
from jax.sharding import PartitionSpec as P

MESH = pl.DeviceIdType.MESH
ROWS = 256
HEADS = 8
HEAD = 128
DOCS = 8
TILES = 8
TOKENS = ROWS // TILES
COLS = TOKENS * HEADS
CTX = 32
WINDOW = 20
LAST = WINDOW // 4
KROWS = ROWS + 16
PIECES = ((0, 128), (128, 144)), ((0, 64), (64, 64))
AHEAD = 3
SLOTS = 4
LEFT_K, RIGHT_K = (2, 10), (18,)
LEFT_V, RIGHT_V = (6, 14), (2, 10, 18)
ACROSS_K, ACROSS_V = (6, 14), ()
NEG = -1e30
SCALE = math.log2(math.e) / math.sqrt(HEAD)


def order_of(column):
    listed = []
    for name in ARRIVAL:
        place, d = "LRoX".index(name[0]), int(name[1])
        slot = 4 * d + (column - (column + (-1, 1, 0, 2)[place]) % 4)
        if 1 <= slot <= WINDOW:
            listed.append(4 * d + place)
    return listed


ARRIVAL = (
    "o1", "L0", "R0", "o2", "L1", "R1", "X0", "o3",
    "L2", "R2", "X1", "o4", "L3", "R3", "X2", "o5",
    "L4", "R4", "X3", "L5", "R5", "X4", "X5",
)
ORDER = [order_of(column) for column in range(4)]


def attend(blocks, first, kbuf, vbuf, qt, top, acc, held_scores):
    at = lax.broadcasted_iota(jnp.int32, (ROWS, HEAD), 0).astype(jnp.float32)
    keys, values = [], []
    for slot, counts_too in blocks:
        below = kbuf[slot, ROWS:, :].astype(jnp.float32)[:1]
        if counts_too is not True:
            below = jnp.where(counts_too, below, float(ROWS))
        before = jnp.where(at < below, 1.0, 0.0).astype(jnp.bfloat16)
        keys.append(jnp.concatenate([kbuf[slot, :ROWS, :], before], axis=1))
        values.append(vbuf[slot])
    rows = ROWS * len(blocks)
    keys = jnp.concatenate(keys, axis=0) if len(blocks) > 1 else keys[0]
    values = jnp.concatenate(values, axis=1) if len(blocks) > 1 else values[0]

    values = jnp.concatenate([values, jnp.ones((16, rows), jnp.bfloat16)], axis=0)

    def scored(j):
        scores = jnp.dot(keys, qt[j], preferred_element_type=jnp.float32)
        if first:
            key = lax.broadcasted_iota(jnp.int32, (ROWS, COLS), 0)
            own = lax.broadcasted_iota(jnp.int32, (1, COLS), 1) // HEADS + j * TOKENS
            scores = jnp.where(key <= own, scores, NEG)
        held_scores[j % SLOTS, :rows] = scores
        return jnp.max(scores, axis=0, keepdims=True) * SCALE

    def add(j, mixed, factor):
        mixed = mixed[:HEAD + 8]
        acc[j] = mixed if first else acc[j] * factor + mixed

    ahead = [scored(j) for j in range(AHEAD)]
    waiting = None
    for j in range(TILES):
        high = ahead.pop(0)
        if j + AHEAD < TILES:
            ahead.append(scored(j + AHEAD))
        factor = None
        if not first:
            high = jnp.maximum(top[j], high)
            factor = jnp.exp2(top[j] - high)
        weights = jnp.exp2(held_scores[j % SLOTS, :rows] * SCALE - high)
        mixed = jnp.dot(values, weights.astype(jnp.bfloat16), preferred_element_type=jnp.float32)
        top[j] = high
        if waiting is not None:
            add(*waiting)
        waiting = (j, mixed, factor)
    add(*waiting)


def kernel(q_hbm, k_hbm, v_hbm, seg_hbm, out_ref, q_ref, v_ref, seg_ref, in_sem, kbuf, vbuf, qt, top, acc, held_scores, turned, stage,
           recv_k, recv_v, send_k, send_v, out_send, out_recv):
    r = lax.axis_index("ctx")
    t = lax.axis_index("tp")
    z, y = r // 4, r % 4
    right = jnp.where(y < 3, r + 1, r - 3)
    left = jnp.where(y > 0, r - 1, r + 3)
    up = jnp.where(z < 7, r + 4, r - 28)
    down = jnp.where(z > 0, r - 4, r + 28)
    to_right = right - r
    to_left = left - r
    reach = jnp.minimum(r, WINDOW)

    barrier = pltpu.get_barrier_semaphore()
    for other in (right, left, up, down, lax.rem(r + 4 * LAST, CTX), lax.rem(r + CTX - 4 * LAST, CTX)):
        pl.semaphore_signal(barrier, inc=1, device_id=(other, t), device_id_type=MESH)
    for step in range(1, TILES):
        pl.semaphore_signal(barrier, inc=1, device_id=(r, lax.rem(t + step, TILES)), device_id_type=MESH)

    taken = [
        pltpu.make_async_copy(seg_hbm, seg_ref, in_sem.at[0]),
        pltpu.make_async_copy(k_hbm, kbuf.at[0, pl.ds(0, ROWS)], in_sem.at[1]),
        pltpu.make_async_copy(v_hbm, v_ref, in_sem.at[2]),
        pltpu.make_async_copy(q_hbm, q_ref, in_sem.at[3]),
    ]
    for copy in taken:
        copy.start()

    taken[0].wait()
    seg = seg_ref[...]
    ids = lax.broadcasted_iota(jnp.int32, (HEAD, ROWS), 0)
    smaller = jnp.where((seg < ids) & (ids < DOCS), 1.0, 0.0).astype(jnp.bfloat16)
    counts = lax.dot_general(jnp.ones((16, ROWS), jnp.bfloat16), smaller, (((1,), (1,)), ((), ())),
                             preferred_element_type=jnp.float32)
    kbuf[0, ROWS:, :] = counts.astype(jnp.bfloat16)
    taken[2].wait()
    vbuf[0] = v_ref[...].T
    taken[1].wait()

    pl.semaphore_wait(barrier, 6 + TILES - 1)

    def moved(part, piece):
        first, size = PIECES[part][piece] if piece is not None else (0, (KROWS, HEAD)[part])
        buffer, sent, landed_at = ((kbuf, send_k, recv_k), (vbuf, send_v, recv_v))[part]

        def copy(src, dst, to, way, d):
            return pltpu.make_async_remote_copy(
                src_ref=buffer.at[src, pl.ds(first, size)], dst_ref=buffer.at[dst, pl.ds(first, size)],
                send_sem=sent.at[way, d], recv_sem=landed_at.at[piece or 0, dst],
                device_id=(to, t), device_id_type=MESH)

        return copy

    def sender(part, piece):
        return lambda *where: moved(part, piece)(*where).start()

    def waiter(part):
        return lambda *where: moved(part, None)(*where).wait_send()

    def inside(slot):
        return (slot >= 1) & (slot <= WINDOW)

    def held(slot):
        return (slot >= 1) & (slot <= reach)

    def clipped(slot):
        return jnp.clip(slot, 0, WINDOW)

    def own_moves(d, act):
        slot = 4 * d
        have = slot <= reach

        @pl.when(have & (z < 7) & (d < LAST - 1))
        def _():
            act(slot, clipped(slot + 4), up, 0, d)

        @pl.when(have & inside(slot + to_right))
        def _():
            act(slot, clipped(slot + to_right), right, 1, d)

        @pl.when(have & inside(slot + to_left))
        def _():
            act(slot, clipped(slot + to_left), left, 2, d)

    def far_moves(act):
        @pl.when(z + LAST <= 7)
        def _():
            act(0, WINDOW, r + 4 * LAST, 5, 0)

    def across_moves(part, d, act):
        slot = across(d)

        @pl.when(held(slot) & (z < 7) & any_of(slot + 4, (ACROSS_K, ACROSS_V)[part]))
        def _():
            act(clipped(slot), clipped(slot + 4), up, 6, d)

    def relay(slot, shift, to, way, d, act, also):
        @pl.when(held(slot) & inside(slot + shift) & also)
        def _():
            act(clipped(slot), clipped(slot + shift), to, way, d)

    def from_left(d):
        return 4 * d - to_left

    def from_right(d):
        return 4 * d - to_right

    def across(d):
        return jnp.where(y >= 2, 4 * d + 2, 4 * d - 2)

    def any_of(slot, slots):
        found = slot < 0
        for other in slots:
            found = found | (slot == other)
        return found

    def left_relays(part, d, act):
        to = from_left(d) + to_right
        also = any_of(to, (LEFT_K, LEFT_V)[part])
        if part == 1:
            also = also | ((to == 2) & (y == 2))
        relay(from_left(d), to_right, right, 3, d, act, also)

    def right_relays(part, d, act):
        relay(from_right(d), to_left, left, 4, d, act, any_of(from_right(d) + to_left, (RIGHT_K, RIGHT_V)[part]))

    def await_piece(part, piece, slot):
        moved(part, piece)(slot, slot, right, 0, 0).wait_recv()

    for part in range(2):
        for piece in range(2):
            own_moves(0, sender(part, piece))
    for part in range(2):
        for piece in range(2):
            far_moves(sender(part, piece))
    taken[3].wait()
    document = jnp.where(seg == ids, NEG, 0.0).astype(jnp.bfloat16)
    for j in range(TILES):
        qt[j, :HEAD] = q_ref[pl.ds(j * COLS, COLS), :].T
        token = lax.broadcasted_iota(jnp.int32, (ROWS, COLS), 0)
        column = lax.broadcasted_iota(jnp.int32, (ROWS, COLS), 1)
        spread = jnp.where(token == column // HEADS + j * TOKENS, 1.0, 0.0).astype(jnp.bfloat16)
        qt[j, HEAD:] = jnp.dot(document, spread, preferred_element_type=jnp.float32).astype(jnp.bfloat16)

    attend([(0, True)], True, kbuf, vbuf, qt, top, acc, held_scores)

    def turn(n):
        pairs = [jnp.int32(0)] * 4
        for column in range(4):
            orders = ORDER[column]
            for m in range(WINDOW // 2):
                pairs[column] = jnp.where(n == m, 32 * orders[2 * m] + orders[2 * m + 1], pairs[column])
        pair = jnp.where(y == 0, pairs[0], jnp.where(y == 1, pairs[1], jnp.where(y == 2, pairs[2], pairs[3])))
        return pair // 32, pair % 32

    def serve(i):
        d, place = i // 4, i % 4
        slot = jnp.where(place == 0, from_left(d), jnp.where(place == 1, from_right(d), jnp.where(
            place == 2, 4 * d, across(d))))
        have = held(slot)
        slot = clipped(slot)

        for at in range(4):
            @pl.when(have & (place == at))
            def _():
                for part in range(2):
                    for piece in range(2):
                        await_piece(part, piece, slot)
                        act = sender(part, piece)
                        if at == 0:
                            left_relays(part, d, act)
                        elif at == 1:
                            right_relays(part, d, act)
                        elif at == 2:
                            own_moves(d, act)
                        else:
                            across_moves(part, d, act)

        return jnp.where(have, slot, 0), have

    def one(n, carry):
        a, b = turn(n)
        slot_a, have_a = serve(a)
        slot_b, have_b = serve(b)

        @pl.when(have_a | have_b)
        def _():
            attend([(slot_a, have_a), (slot_b, have_b)], False, kbuf, vbuf, qt, top, acc, held_scores)

        return carry

    lax.fori_loop(0, WINDOW // 2, one, 0)

    def out_copy(j):
        return pltpu.make_async_remote_copy(
            src_ref=stage.at[j], dst_ref=out_ref.at[:, pl.ds(pl.multiple_of(t * COLS * 4, COLS * 4), COLS * 4)],
            send_sem=out_send.at[j], recv_sem=out_recv.at[t], device_id=(r, j), device_id_type=MESH)

    def finish(step, carry):
        j = lax.rem(t + 1 + step, TILES)
        whole = acc[j, :HEAD] / acc[j, HEAD:HEAD + 1]
        turned[...] = whole.T
        for h in range(HEADS):
            stage[j, :, h * HEAD:(h + 1) * HEAD] = turned[pl.ds(h, TOKENS, stride=HEADS), :].astype(jnp.bfloat16)

        @pl.when(step > 0)
        def _():
            out_copy(lax.rem(t + step, TILES)).start()

        return carry

    lax.fori_loop(0, TILES, finish, 0)
    out_ref[:, pl.ds(pl.multiple_of(t * COLS * 4, COLS * 4), COLS * 4)] = stage[t]

    def settle(d, carry):
        for part in range(2):
            own_moves(d, waiter(part))
            across_moves(part, d, waiter(part))
            left_relays(part, d, waiter(part))
            right_relays(part, d, waiter(part))
        return carry

    lax.fori_loop(0, LAST + 1, settle, 0)
    for part in range(2):
        far_moves(waiter(part))

    def landed(step, carry):
        j = lax.rem(t + step, TILES)
        out_copy(j).wait_send()
        pltpu.make_async_remote_copy(
            src_ref=stage.at[j],
            dst_ref=out_ref.at[:, pl.ds(pl.multiple_of(j * COLS * 4, COLS * 4), COLS * 4)],
            send_sem=out_send.at[j], recv_sem=out_recv.at[j], device_id=(r, j), device_id_type=MESH).wait_recv()
        return carry

    lax.fori_loop(1, TILES, landed, 0)


def local(queries, keys, values, segment_ids):
    rows, heads, head = queries.shape
    vmem = pl.BlockSpec(memory_space=pltpu.VMEM)
    return pl.pallas_call(
        kernel,
        out_shape=pltpu.VMEM((TOKENS, TILES * heads * head), jnp.bfloat16),
        in_specs=[pl.BlockSpec(memory_space=pl.ANY)] * 4,
        out_specs=vmem,
        scratch_shapes=[
            pltpu.VMEM((COLS * TILES, HEAD), jnp.bfloat16),
            pltpu.VMEM((ROWS, HEAD), jnp.bfloat16),
            pltpu.VMEM((1, ROWS), jnp.int32),
            pltpu.SemaphoreType.DMA((4,)),
            pltpu.VMEM((WINDOW + 1, KROWS, HEAD), jnp.bfloat16),
            pltpu.VMEM((WINDOW + 1, HEAD, ROWS), jnp.bfloat16),
            pltpu.VMEM((TILES, 2 * HEAD, COLS), jnp.bfloat16),
            pltpu.VMEM((TILES, 1, COLS), jnp.float32),
            pltpu.VMEM((TILES, HEAD + 8, COLS), jnp.float32),
            pltpu.VMEM((SLOTS, 2 * ROWS, COLS), jnp.float32),
            pltpu.VMEM((COLS, HEAD), jnp.float32),
            pltpu.VMEM((TILES, TOKENS, HEADS * HEAD), jnp.bfloat16),
            pltpu.SemaphoreType.DMA((2, WINDOW + 1)),
            pltpu.SemaphoreType.DMA((2, WINDOW + 1)),
            pltpu.SemaphoreType.DMA((7, LAST + 1)),
            pltpu.SemaphoreType.DMA((7, LAST + 1)),
            pltpu.SemaphoreType.DMA((TILES,)),
            pltpu.SemaphoreType.DMA((TILES,)),
        ],
        compiler_params=pltpu.CompilerParams(collective_id=0, has_side_effects=True),
    )(queries.reshape(rows * heads, head), keys.reshape(rows, head), values.reshape(rows, head),
      segment_ids.reshape(1, rows))


def solution(mesh):
    in_specs = (P("ctx", "tp", None), P("ctx", "tp", None), P("ctx", "tp", None), P("ctx"))
    out_specs = P(("ctx", "tp"), None)
    return jax.shard_map(local, mesh=mesh, in_specs=in_specs, out_specs=out_specs, check_vma=False)
```

```python
import functools
import math

import jax
import jax.numpy as jnp
from jax import lax
from jax.experimental import pallas as pl
from jax.experimental.pallas import tpu as pltpu
from jax.sharding import PartitionSpec as P

MESH = pl.DeviceIdType.MESH
ROWS = 256
HEADS = 8
HEAD = 128
DOCS = 8
TILES = 8
TOKENS = ROWS // TILES
COLS = TOKENS * HEADS
CTX = 32
WINDOW = 20
LAST = WINDOW // 4
KROWS = ROWS + 16
PIECES = ((0, 128), (128, 144)), ((0, 64), (64, 64))
AHEAD = 3
SLOTS = 4
LEFT_K, RIGHT_K = (2, 10), (18,)
LEFT_V, RIGHT_V = (6, 14), (2, 10, 18)
ACROSS_K, ACROSS_V = (6, 14), ()
NEG = -1e30
SCALE = math.log2(math.e) / math.sqrt(HEAD)


def order_of(column):
    listed = []
    for name in ARRIVAL:
        place, d = "LRoX".index(name[0]), int(name[1])
        slot = 4 * d + (column - (column + (-1, 1, 0, 2)[place]) % 4)
        if 1 <= slot <= WINDOW:
            listed.append(4 * d + place)
    return listed


ARRIVAL = (
    "o1", "L0", "R0", "o2", "L1", "R1", "X0", "o3",
    "L2", "R2", "X1", "o4", "L3", "R3", "X2", "o5",
    "L4", "R4", "X3", "L5", "R5", "X4", "X5",
)
ORDER = [order_of(column) for column in range(4)]


def attend(blocks, first, kbuf, vbuf, qt, top, acc, held_scores):
    at = lax.broadcasted_iota(jnp.int32, (ROWS, HEAD), 0).astype(jnp.float32)
    keys, values = [], []
    for slot, counts_too in blocks:
        below = kbuf[slot, ROWS:, :].astype(jnp.float32)[:1]
        if counts_too is not True:
            below = jnp.where(counts_too, below, float(ROWS))
        before = jnp.where(at < below, 1.0, 0.0).astype(jnp.bfloat16)
        keys.append(jnp.concatenate([kbuf[slot, :ROWS, :], before], axis=1))
        values.append(vbuf[slot])
    rows = ROWS * len(blocks)
    keys = jnp.concatenate(keys, axis=0) if len(blocks) > 1 else keys[0]
    values = jnp.concatenate(values, axis=1) if len(blocks) > 1 else values[0]

    values = jnp.concatenate([values, jnp.ones((16, rows), jnp.bfloat16)], axis=0)

    def scored(j):
        scores = jnp.dot(keys, qt[j], preferred_element_type=jnp.float32)
        if first:
            key = lax.broadcasted_iota(jnp.int32, (ROWS, COLS), 0)
            own = lax.broadcasted_iota(jnp.int32, (1, COLS), 1) // HEADS + j * TOKENS
            scores = jnp.where(key <= own, scores, NEG)
        held_scores[j % SLOTS, :rows] = scores
        return jnp.max(scores, axis=0, keepdims=True) * SCALE

    def add(j, mixed, factor):
        mixed = mixed[:HEAD + 8]
        acc[j] = mixed if first else acc[j] * factor + mixed

    ahead = [scored(j) for j in range(AHEAD)]
    waiting = None
    for j in range(TILES):
        high = ahead.pop(0)
        if j + AHEAD < TILES:
            ahead.append(scored(j + AHEAD))
        factor = None
        if not first:
            high = jnp.maximum(top[j], high)
            factor = jnp.exp2(top[j] - high)
        weights = jnp.exp2(held_scores[j % SLOTS, :rows] * SCALE - high)
        mixed = jnp.dot(values, weights.astype(jnp.bfloat16), preferred_element_type=jnp.float32)
        top[j] = high
        if waiting is not None:
            add(*waiting)
        waiting = (j, mixed, factor)
    add(*waiting)


def kernel(q_hbm, k_hbm, v_hbm, seg_hbm, out_ref, q_ref, v_ref, seg_ref, in_sem, kbuf, vbuf, qt, top, acc, held_scores, turned, stage,
           recv_k, recv_v, send_k, send_v, out_send, out_recv):
    r = lax.axis_index("ctx")
    t = lax.axis_index("tp")
    z, y = r // 4, r % 4
    right = jnp.where(y < 3, r + 1, r - 3)
    left = jnp.where(y > 0, r - 1, r + 3)
    up = jnp.where(z < 7, r + 4, r - 28)
    down = jnp.where(z > 0, r - 4, r + 28)
    to_right = right - r
    to_left = left - r
    reach = jnp.minimum(r, WINDOW)

    barrier = pltpu.get_barrier_semaphore()
    for other in (right, left, up, down, lax.rem(r + 4 * LAST, CTX), lax.rem(r + CTX - 4 * LAST, CTX)):
        pl.semaphore_signal(barrier, inc=1, device_id=(other, t), device_id_type=MESH)
    for step in range(1, TILES):
        pl.semaphore_signal(barrier, inc=1, device_id=(r, lax.rem(t + step, TILES)), device_id_type=MESH)

    taken = [
        pltpu.make_async_copy(seg_hbm, seg_ref, in_sem.at[0]),
        pltpu.make_async_copy(k_hbm, kbuf.at[0, pl.ds(0, ROWS)], in_sem.at[1]),
        pltpu.make_async_copy(v_hbm, v_ref, in_sem.at[2]),
        pltpu.make_async_copy(q_hbm, q_ref, in_sem.at[3]),
    ]
    for copy in taken:
        copy.start()

    taken[0].wait()
    seg = seg_ref[...]
    ids = lax.broadcasted_iota(jnp.int32, (HEAD, ROWS), 0)
    smaller = jnp.where((seg < ids) & (ids < DOCS), 1.0, 0.0).astype(jnp.bfloat16)
    counts = lax.dot_general(jnp.ones((16, ROWS), jnp.bfloat16), smaller, (((1,), (1,)), ((), ())),
                             preferred_element_type=jnp.float32)
    kbuf[0, ROWS:, :] = counts.astype(jnp.bfloat16)
    taken[2].wait()
    vbuf[0] = v_ref[...].T
    taken[1].wait()

    pl.semaphore_wait(barrier, 6 + TILES - 1)

    def moved(part, piece):
        first, size = PIECES[part][piece] if piece is not None else (0, (KROWS, HEAD)[part])
        buffer, sent, landed_at = ((kbuf, send_k, recv_k), (vbuf, send_v, recv_v))[part]

        def copy(src, dst, to, way, d):
            return pltpu.make_async_remote_copy(
                src_ref=buffer.at[src, pl.ds(first, size)], dst_ref=buffer.at[dst, pl.ds(first, size)],
                send_sem=sent.at[way, d], recv_sem=landed_at.at[piece or 0, dst],
                device_id=(to, t), device_id_type=MESH)

        return copy

    def sender(part, piece):
        return lambda *where: moved(part, piece)(*where).start()

    def waiter(part):
        return lambda *where: moved(part, None)(*where).wait_send()

    def inside(slot):
        return (slot >= 1) & (slot <= WINDOW)

    def held(slot):
        return (slot >= 1) & (slot <= reach)

    def clipped(slot):
        return jnp.clip(slot, 0, WINDOW)

    def own_moves(d, act):
        slot = 4 * d
        have = slot <= reach

        @pl.when(have & (z < 7) & (d < LAST - 1))
        def _():
            act(slot, clipped(slot + 4), up, 0, d)

        @pl.when(have & inside(slot + to_right))
        def _():
            act(slot, clipped(slot + to_right), right, 1, d)

        @pl.when(have & inside(slot + to_left))
        def _():
            act(slot, clipped(slot + to_left), left, 2, d)

    def far_moves(act):
        @pl.when(z + LAST <= 7)
        def _():
            act(0, WINDOW, r + 4 * LAST, 5, 0)

    def across_moves(part, d, act):
        slot = across(d)

        @pl.when(held(slot) & (z < 7) & any_of(slot + 4, (ACROSS_K, ACROSS_V)[part]))
        def _():
            act(clipped(slot), clipped(slot + 4), up, 6, d)

    def relay(slot, shift, to, way, d, act, also):
        @pl.when(held(slot) & inside(slot + shift) & also)
        def _():
            act(clipped(slot), clipped(slot + shift), to, way, d)

    def from_left(d):
        return 4 * d - to_left

    def from_right(d):
        return 4 * d - to_right

    def across(d):
        return jnp.where(y >= 2, 4 * d + 2, 4 * d - 2)

    def any_of(slot, slots):
        found = slot < 0
        for other in slots:
            found = found | (slot == other)
        return found

    def left_relays(part, d, act):
        to = from_left(d) + to_right
        also = any_of(to, (LEFT_K, LEFT_V)[part])
        if part == 1:
            also = also | ((to == 2) & (y == 2))
        relay(from_left(d), to_right, right, 3, d, act, also)

    def right_relays(part, d, act):
        relay(from_right(d), to_left, left, 4, d, act, any_of(from_right(d) + to_left, (RIGHT_K, RIGHT_V)[part]))

    def await_piece(part, piece, slot):
        moved(part, piece)(slot, slot, right, 0, 0).wait_recv()

    for part in range(2):
        for piece in range(2):
            own_moves(0, sender(part, piece))
    for part in range(2):
        for piece in range(2):
            far_moves(sender(part, piece))
    taken[3].wait()
    document = jnp.where(seg == ids, NEG, 0.0).astype(jnp.bfloat16)
    for j in range(TILES):
        qt[j, :HEAD] = q_ref[pl.ds(j * COLS, COLS), :].T
        token = lax.broadcasted_iota(jnp.int32, (ROWS, COLS), 0)
        column = lax.broadcasted_iota(jnp.int32, (ROWS, COLS), 1)
        spread = jnp.where(token == column // HEADS + j * TOKENS, 1.0, 0.0).astype(jnp.bfloat16)
        qt[j, HEAD:] = jnp.dot(document, spread, preferred_element_type=jnp.float32).astype(jnp.bfloat16)

    attend([(0, True)], True, kbuf, vbuf, qt, top, acc, held_scores)

    def turn(n):
        pairs = [jnp.int32(0)] * 4
        for column in range(4):
            orders = ORDER[column]
            for m in range(WINDOW // 2):
                pairs[column] = jnp.where(n == m, 32 * orders[2 * m] + orders[2 * m + 1], pairs[column])
        pair = jnp.where(y == 0, pairs[0], jnp.where(y == 1, pairs[1], jnp.where(y == 2, pairs[2], pairs[3])))
        return pair // 32, pair % 32

    def serve(i):
        d, place = i // 4, i % 4
        slot = jnp.where(place == 0, from_left(d), jnp.where(place == 1, from_right(d), jnp.where(
            place == 2, 4 * d, across(d))))
        have = held(slot)
        slot = clipped(slot)

        for at in range(4):
            @pl.when(have & (place == at))
            def _():
                for part in range(2):
                    for piece in range(2):
                        await_piece(part, piece, slot)
                        act = sender(part, piece)
                        if at == 0:
                            left_relays(part, d, act)
                        elif at == 1:
                            right_relays(part, d, act)
                        elif at == 2:
                            own_moves(d, act)
                        else:
                            across_moves(part, d, act)

        return jnp.where(have, slot, 0), have

    def one(n, carry):
        a, b = turn(n)
        slot_a, have_a = serve(a)
        slot_b, have_b = serve(b)

        @pl.when(have_a | have_b)
        def _():
            attend([(slot_a, have_a), (slot_b, have_b)], False, kbuf, vbuf, qt, top, acc, held_scores)

        return carry

    lax.fori_loop(0, WINDOW // 2, one, 0)

    def out_copy(j):
        return pltpu.make_async_remote_copy(
            src_ref=stage.at[j], dst_ref=out_ref.at[:, pl.ds(pl.multiple_of(t * COLS * 4, COLS * 4), COLS * 4)],
            send_sem=out_send.at[j], recv_sem=out_recv.at[t], device_id=(r, j), device_id_type=MESH)

    def partner(step):
        ahead = jnp.where(step < 2, 2, jnp.where(step < 6, 1 + 2 * (step % 2), 0))
        other = jnp.where(step < 2, step, jnp.where(step < 6, (step - 2) // 2, 7 - step))
        return (t // 2 + ahead) % 4 * 2 + (t + other) % 2

    def finish(step, carry):
        j = partner(step)
        whole = acc[j, :HEAD] / acc[j, HEAD:HEAD + 1]
        turned[...] = whole.T
        for h in range(HEADS):
            stage[j, :, h * HEAD:(h + 1) * HEAD] = turned[pl.ds(h, TOKENS, stride=HEADS), :].astype(jnp.bfloat16)

        @pl.when(step > 0)
        def _():
            out_copy(partner(step - 1)).start()

        return carry

    lax.fori_loop(0, TILES, finish, 0)
    out_ref[:, pl.ds(pl.multiple_of(t * COLS * 4, COLS * 4), COLS * 4)] = stage[t]

    def settle(d, carry):
        for part in range(2):
            own_moves(d, waiter(part))
            across_moves(part, d, waiter(part))
            left_relays(part, d, waiter(part))
            right_relays(part, d, waiter(part))
        return carry

    lax.fori_loop(0, LAST + 1, settle, 0)
    for part in range(2):
        far_moves(waiter(part))

    def landed(step, carry):
        j = lax.rem(t + step, TILES)
        out_copy(j).wait_send()
        pltpu.make_async_remote_copy(
            src_ref=stage.at[j],
            dst_ref=out_ref.at[:, pl.ds(pl.multiple_of(j * COLS * 4, COLS * 4), COLS * 4)],
            send_sem=out_send.at[j], recv_sem=out_recv.at[j], device_id=(r, j), device_id_type=MESH).wait_recv()
        return carry

    lax.fori_loop(1, TILES, landed, 0)


def local(queries, keys, values, segment_ids):
    rows, heads, head = queries.shape
    vmem = pl.BlockSpec(memory_space=pltpu.VMEM)
    return pl.pallas_call(
        kernel,
        out_shape=pltpu.VMEM((TOKENS, TILES * heads * head), jnp.bfloat16),
        in_specs=[pl.BlockSpec(memory_space=pl.ANY)] * 4,
        out_specs=vmem,
        scratch_shapes=[
            pltpu.VMEM((COLS * TILES, HEAD), jnp.bfloat16),
            pltpu.VMEM((ROWS, HEAD), jnp.bfloat16),
            pltpu.VMEM((1, ROWS), jnp.int32),
            pltpu.SemaphoreType.DMA((4,)),
            pltpu.VMEM((WINDOW + 1, KROWS, HEAD), jnp.bfloat16),
            pltpu.VMEM((WINDOW + 1, HEAD, ROWS), jnp.bfloat16),
            pltpu.VMEM((TILES, 2 * HEAD, COLS), jnp.bfloat16),
            pltpu.VMEM((TILES, 1, COLS), jnp.float32),
            pltpu.VMEM((TILES, HEAD + 8, COLS), jnp.float32),
            pltpu.VMEM((SLOTS, 2 * ROWS, COLS), jnp.float32),
            pltpu.VMEM((COLS, HEAD), jnp.float32),
            pltpu.VMEM((TILES, TOKENS, HEADS * HEAD), jnp.bfloat16),
            pltpu.SemaphoreType.DMA((2, WINDOW + 1)),
            pltpu.SemaphoreType.DMA((2, WINDOW + 1)),
            pltpu.SemaphoreType.DMA((7, LAST + 1)),
            pltpu.SemaphoreType.DMA((7, LAST + 1)),
            pltpu.SemaphoreType.DMA((TILES,)),
            pltpu.SemaphoreType.DMA((TILES,)),
        ],
        compiler_params=pltpu.CompilerParams(collective_id=0, has_side_effects=True),
    )(queries.reshape(rows * heads, head), keys.reshape(rows, head), values.reshape(rows, head),
      segment_ids.reshape(1, rows))


def solution(mesh):
    in_specs = (P("ctx", "tp", None), P("ctx", "tp", None), P("ctx", "tp", None), P("ctx"))
    out_specs = P(("ctx", "tp"), None)
    return jax.shard_map(local, mesh=mesh, in_specs=in_specs, out_specs=out_specs, check_vma=False)
```

```python
import functools
import math

import jax
import jax.numpy as jnp
from jax import lax
from jax.experimental import pallas as pl
from jax.experimental.pallas import tpu as pltpu
from jax.sharding import PartitionSpec as P

MESH = pl.DeviceIdType.MESH
ROWS = 256
HEADS = 8
HEAD = 128
DOCS = 8
TILES = 8
TOKENS = ROWS // TILES
COLS = TOKENS * HEADS
CTX = 32
WINDOW = 20
LAST = WINDOW // 4
KROWS = ROWS + 16
PIECES = ((0, 128), (128, 144)), ((0, 64), (64, 64))
AHEAD = 3
SLOTS = 4
LEFT_K, RIGHT_K = (2, 10), (18,)
LEFT_V, RIGHT_V = (6, 14), (2, 10, 18)
ACROSS_K, ACROSS_V = (6, 14), ()
NEG = -1e30
SCALE = math.log2(math.e) / math.sqrt(HEAD)


def order_of(column):
    listed = []
    for name in ARRIVAL:
        place, d = "LRoX".index(name[0]), int(name[1])
        slot = 4 * d + (column - (column + (-1, 1, 0, 2)[place]) % 4)
        if 1 <= slot <= WINDOW:
            listed.append(4 * d + place)
    return listed


ARRIVAL = (
    "o1", "L0", "R0", "o2", "L1", "R1", "X0", "o3",
    "L2", "R2", "X1", "o4", "L3", "R3", "X2", "o5",
    "L4", "R4", "X3", "L5", "R5", "X4", "X5",
)
ORDER = [order_of(column) for column in range(4)]


def attend(blocks, first, kbuf, vbuf, qt, top, acc, held_scores):
    at = lax.broadcasted_iota(jnp.int32, (ROWS, HEAD), 0).astype(jnp.float32)
    keys, values = [], []
    for slot, counts_too in blocks:
        below = kbuf[slot, ROWS:, :].astype(jnp.float32)[:1]
        if counts_too is not True:
            below = jnp.where(counts_too, below, float(ROWS))
        before = jnp.where(at < below, 1.0, 0.0).astype(jnp.bfloat16)
        keys.append(jnp.concatenate([kbuf[slot, :ROWS, :], before], axis=1))
        values.append(vbuf[slot])
    rows = ROWS * len(blocks)
    keys = jnp.concatenate(keys, axis=0) if len(blocks) > 1 else keys[0]
    values = jnp.concatenate(values, axis=1) if len(blocks) > 1 else values[0]

    values = jnp.concatenate([values, jnp.ones((16, rows), jnp.bfloat16)], axis=0)

    def scored(j):
        scores = jnp.dot(keys, qt[j], preferred_element_type=jnp.float32)
        if first:
            key = lax.broadcasted_iota(jnp.int32, (ROWS, COLS), 0)
            own = lax.broadcasted_iota(jnp.int32, (1, COLS), 1) // HEADS + j * TOKENS
            scores = jnp.where(key <= own, scores, NEG)
        held_scores[j % SLOTS, :rows] = scores
        return jnp.max(scores, axis=0, keepdims=True) * SCALE

    def add(j, mixed, factor):
        mixed = mixed[:HEAD + 8]
        acc[j] = mixed if first else acc[j] * factor + mixed

    ahead = [scored(j) for j in range(AHEAD)]
    waiting = None
    for j in range(TILES):
        high = ahead.pop(0)
        if j + AHEAD < TILES:
            ahead.append(scored(j + AHEAD))
        factor = None
        if not first:
            high = jnp.maximum(top[j], high)
            factor = jnp.exp2(top[j] - high)
        weights = jnp.exp2(held_scores[j % SLOTS, :rows] * SCALE - high)
        mixed = jnp.dot(values, weights.astype(jnp.bfloat16), preferred_element_type=jnp.float32)
        top[j] = high
        if waiting is not None:
            add(*waiting)
        waiting = (j, mixed, factor)
    add(*waiting)


def kernel(q_hbm, k_hbm, v_hbm, seg_hbm, out_ref, q_ref, v_ref, seg_ref, in_sem, kbuf, vbuf, qt, top, acc, held_scores, turned, stage,
           recv_k, recv_v, send_k, send_v, out_send, out_recv):
    r = lax.axis_index("ctx")
    t = lax.axis_index("tp")
    z, y = r // 4, r % 4
    right = jnp.where(y < 3, r + 1, r - 3)
    left = jnp.where(y > 0, r - 1, r + 3)
    up = jnp.where(z < 7, r + 4, r - 28)
    down = jnp.where(z > 0, r - 4, r + 28)
    to_right = right - r
    to_left = left - r
    reach = jnp.minimum(r, WINDOW)

    barrier = pltpu.get_barrier_semaphore()
    for other in (right, left, up, down, lax.rem(r + 4 * LAST, CTX), lax.rem(r + CTX - 4 * LAST, CTX)):
        pl.semaphore_signal(barrier, inc=1, device_id=(other, t), device_id_type=MESH)
    for step in range(1, TILES):
        pl.semaphore_signal(barrier, inc=1, device_id=(r, lax.rem(t + step, TILES)), device_id_type=MESH)

    taken = [
        pltpu.make_async_copy(seg_hbm, seg_ref, in_sem.at[0]),
        pltpu.make_async_copy(k_hbm, kbuf.at[0, pl.ds(0, ROWS)], in_sem.at[1]),
        pltpu.make_async_copy(v_hbm, v_ref, in_sem.at[2]),
        pltpu.make_async_copy(q_hbm, q_ref, in_sem.at[3]),
    ]
    for copy in taken:
        copy.start()

    taken[0].wait()
    seg = seg_ref[...]
    ids = lax.broadcasted_iota(jnp.int32, (HEAD, ROWS), 0)
    smaller = jnp.where((seg < ids) & (ids < DOCS), 1.0, 0.0).astype(jnp.bfloat16)
    counts = lax.dot_general(jnp.ones((16, ROWS), jnp.bfloat16), smaller, (((1,), (1,)), ((), ())),
                             preferred_element_type=jnp.float32)
    kbuf[0, ROWS:, :] = counts.astype(jnp.bfloat16)
    taken[2].wait()
    vbuf[0] = v_ref[...].T
    taken[1].wait()

    pl.semaphore_wait(barrier, 6 + TILES - 1)

    def moved(part, piece):
        first, size = PIECES[part][piece] if piece is not None else (0, (KROWS, HEAD)[part])
        buffer, sent, landed_at = ((kbuf, send_k, recv_k), (vbuf, send_v, recv_v))[part]

        def copy(src, dst, to, way, d):
            return pltpu.make_async_remote_copy(
                src_ref=buffer.at[src, pl.ds(first, size)], dst_ref=buffer.at[dst, pl.ds(first, size)],
                send_sem=sent.at[way, d], recv_sem=landed_at.at[piece or 0, dst],
                device_id=(to, t), device_id_type=MESH)

        return copy

    def sender(part, piece):
        return lambda *where: moved(part, piece)(*where).start()

    def waiter(part):
        return lambda *where: moved(part, None)(*where).wait_send()

    def inside(slot):
        return (slot >= 1) & (slot <= WINDOW)

    def held(slot):
        return (slot >= 1) & (slot <= reach)

    def clipped(slot):
        return jnp.clip(slot, 0, WINDOW)

    def own_moves(d, act):
        slot = 4 * d
        have = slot <= reach

        @pl.when(have & inside(slot + to_right))
        def _():
            act(slot, clipped(slot + to_right), right, 1, d)

        @pl.when(have & inside(slot + to_left))
        def _():
            act(slot, clipped(slot + to_left), left, 2, d)

        @pl.when(have & (z < 7) & (d < LAST - 1))
        def _():
            act(slot, clipped(slot + 4), up, 0, d)

    def far_moves(act):
        @pl.when(z + LAST <= 7)
        def _():
            act(0, WINDOW, r + 4 * LAST, 5, 0)

    def across_moves(part, d, act):
        slot = across(d)

        @pl.when(held(slot) & (z < 7) & any_of(slot + 4, (ACROSS_K, ACROSS_V)[part]))
        def _():
            act(clipped(slot), clipped(slot + 4), up, 6, d)

    def relay(slot, shift, to, way, d, act, also):
        @pl.when(held(slot) & inside(slot + shift) & also)
        def _():
            act(clipped(slot), clipped(slot + shift), to, way, d)

    def from_left(d):
        return 4 * d - to_left

    def from_right(d):
        return 4 * d - to_right

    def across(d):
        return jnp.where(y >= 2, 4 * d + 2, 4 * d - 2)

    def any_of(slot, slots):
        found = slot < 0
        for other in slots:
            found = found | (slot == other)
        return found

    def left_relays(part, d, act):
        to = from_left(d) + to_right
        also = any_of(to, (LEFT_K, LEFT_V)[part])
        if part == 1:
            also = also | ((to == 2) & (y == 2))
        relay(from_left(d), to_right, right, 3, d, act, also)

    def right_relays(part, d, act):
        relay(from_right(d), to_left, left, 4, d, act, any_of(from_right(d) + to_left, (RIGHT_K, RIGHT_V)[part]))

    def await_piece(part, piece, slot):
        moved(part, piece)(slot, slot, right, 0, 0).wait_recv()

    for part in range(2):
        for piece in range(2):
            own_moves(0, sender(part, piece))
    for part in range(2):
        for piece in range(2):
            far_moves(sender(part, piece))
    taken[3].wait()
    document = jnp.where(seg == ids, NEG, 0.0).astype(jnp.bfloat16)
    for j in range(TILES):
        qt[j, :HEAD] = q_ref[pl.ds(j * COLS, COLS), :].T
        token = lax.broadcasted_iota(jnp.int32, (ROWS, COLS), 0)
        column = lax.broadcasted_iota(jnp.int32, (ROWS, COLS), 1)
        spread = jnp.where(token == column // HEADS + j * TOKENS, 1.0, 0.0).astype(jnp.bfloat16)
        qt[j, HEAD:] = jnp.dot(document, spread, preferred_element_type=jnp.float32).astype(jnp.bfloat16)

    attend([(0, True)], True, kbuf, vbuf, qt, top, acc, held_scores)

    def turn(n):
        pairs = [jnp.int32(0)] * 4
        for column in range(4):
            orders = ORDER[column]
            for m in range(WINDOW // 2):
                pairs[column] = jnp.where(n == m, 32 * orders[2 * m] + orders[2 * m + 1], pairs[column])
        pair = jnp.where(y == 0, pairs[0], jnp.where(y == 1, pairs[1], jnp.where(y == 2, pairs[2], pairs[3])))
        return pair // 32, pair % 32

    def serve(i):
        d, place = i // 4, i % 4
        slot = jnp.where(place == 0, from_left(d), jnp.where(place == 1, from_right(d), jnp.where(
            place == 2, 4 * d, across(d))))
        have = held(slot)
        slot = clipped(slot)

        for at in range(4):
            @pl.when(have & (place == at))
            def _():
                for part in range(2):
                    for piece in range(2):
                        await_piece(part, piece, slot)
                        act = sender(part, piece)
                        if at == 0:
                            left_relays(part, d, act)
                        elif at == 1:
                            right_relays(part, d, act)
                        elif at == 2:
                            own_moves(d, act)
                        else:
                            across_moves(part, d, act)

        return jnp.where(have, slot, 0), have

    def one(n, carry):
        a, b = turn(n)
        slot_a, have_a = serve(a)
        slot_b, have_b = serve(b)

        @pl.when(have_a | have_b)
        def _():
            attend([(slot_a, have_a), (slot_b, have_b)], False, kbuf, vbuf, qt, top, acc, held_scores)

        return carry

    lax.fori_loop(0, WINDOW // 2, one, 0)

    def out_copy(j):
        return pltpu.make_async_remote_copy(
            src_ref=stage.at[j], dst_ref=out_ref.at[:, pl.ds(pl.multiple_of(t * COLS * 4, COLS * 4), COLS * 4)],
            send_sem=out_send.at[j], recv_sem=out_recv.at[t], device_id=(r, j), device_id_type=MESH)

    def partner(step):
        ahead = jnp.where(step < 2, 2, jnp.where(step < 6, 1 + 2 * (step % 2), 0))
        other = jnp.where(step < 2, step, jnp.where(step < 6, (step - 2) // 2, 7 - step))
        return (t // 2 + ahead) % 4 * 2 + (t + other) % 2

    def finish(step, carry):
        j = partner(step)
        whole = acc[j, :HEAD] / acc[j, HEAD:HEAD + 1]
        turned[...] = whole.T
        for h in range(HEADS):
            stage[j, :, h * HEAD:(h + 1) * HEAD] = turned[pl.ds(h, TOKENS, stride=HEADS), :].astype(jnp.bfloat16)

        @pl.when(step > 0)
        def _():
            out_copy(partner(step - 1)).start()

        return carry

    lax.fori_loop(0, TILES, finish, 0)
    out_ref[:, pl.ds(pl.multiple_of(t * COLS * 4, COLS * 4), COLS * 4)] = stage[t]

    def settle(d, carry):
        for part in range(2):
            own_moves(d, waiter(part))
            across_moves(part, d, waiter(part))
            left_relays(part, d, waiter(part))
            right_relays(part, d, waiter(part))
        return carry

    lax.fori_loop(0, LAST + 1, settle, 0)
    for part in range(2):
        far_moves(waiter(part))

    def landed(step, carry):
        j = lax.rem(t + step, TILES)
        out_copy(j).wait_send()
        pltpu.make_async_remote_copy(
            src_ref=stage.at[j],
            dst_ref=out_ref.at[:, pl.ds(pl.multiple_of(j * COLS * 4, COLS * 4), COLS * 4)],
            send_sem=out_send.at[j], recv_sem=out_recv.at[j], device_id=(r, j), device_id_type=MESH).wait_recv()
        return carry

    lax.fori_loop(1, TILES, landed, 0)


def local(queries, keys, values, segment_ids):
    rows, heads, head = queries.shape
    vmem = pl.BlockSpec(memory_space=pltpu.VMEM)
    return pl.pallas_call(
        kernel,
        out_shape=pltpu.VMEM((TOKENS, TILES * heads * head), jnp.bfloat16),
        in_specs=[pl.BlockSpec(memory_space=pl.ANY)] * 4,
        out_specs=vmem,
        scratch_shapes=[
            pltpu.VMEM((COLS * TILES, HEAD), jnp.bfloat16),
            pltpu.VMEM((ROWS, HEAD), jnp.bfloat16),
            pltpu.VMEM((1, ROWS), jnp.int32),
            pltpu.SemaphoreType.DMA((4,)),
            pltpu.VMEM((WINDOW + 1, KROWS, HEAD), jnp.bfloat16),
            pltpu.VMEM((WINDOW + 1, HEAD, ROWS), jnp.bfloat16),
            pltpu.VMEM((TILES, 2 * HEAD, COLS), jnp.bfloat16),
            pltpu.VMEM((TILES, 1, COLS), jnp.float32),
            pltpu.VMEM((TILES, HEAD + 8, COLS), jnp.float32),
            pltpu.VMEM((SLOTS, 2 * ROWS, COLS), jnp.float32),
            pltpu.VMEM((COLS, HEAD), jnp.float32),
            pltpu.VMEM((TILES, TOKENS, HEADS * HEAD), jnp.bfloat16),
            pltpu.SemaphoreType.DMA((2, WINDOW + 1)),
            pltpu.SemaphoreType.DMA((2, WINDOW + 1)),
            pltpu.SemaphoreType.DMA((7, LAST + 1)),
            pltpu.SemaphoreType.DMA((7, LAST + 1)),
            pltpu.SemaphoreType.DMA((TILES,)),
            pltpu.SemaphoreType.DMA((TILES,)),
        ],
        compiler_params=pltpu.CompilerParams(collective_id=0, has_side_effects=True),
    )(queries.reshape(rows * heads, head), keys.reshape(rows, head), values.reshape(rows, head),
      segment_ids.reshape(1, rows))


def solution(mesh):
    in_specs = (P("ctx", "tp", None), P("ctx", "tp", None), P("ctx", "tp", None), P("ctx"))
    out_specs = P(("ctx", "tp"), None)
    return jax.shard_map(local, mesh=mesh, in_specs=in_specs, out_specs=out_specs, check_vma=False)
```
